256 devices in a mesh: grp: 2 (over y), row: 32 (over z, core), col: 4 (over x).
Axes of the slice: x: 4, y: 2, z: 16, core: 2. Of those that a mesh axis runs over, the one named last changes fastest.
The devices are a block of a 4x16x16 slice.
Arguments:
- pair: bfloat16 [768, 384, 128], P(('grp', 'row'), 'col'), parts along dimension 0, may hold values from -6 to 6
- token_count: int32 [2], P('grp'), parts along dimension 0, may hold values from 288 to 384
- tri_in: bfloat16 [2, 128, 512], replicated, may hold values from -0.5 to 0.5
- tri_gate: bfloat16 [2, 128, 128], replicated, may hold values from -0.5 to 0.5
- tri_out: bfloat16 [2, 128, 128], replicated, may hold values from -0.5 to 0.5
- trans_in: bfloat16 [128, 1024], replicated, may hold values from -0.5 to 0.5
- trans_out: bfloat16 [512, 128], replicated, may hold values from -0.25 to 0.25
Outputs:
- pair_out: bfloat16 [768, 384, 128], P(('grp', 'row'), 'col'), parts along dimension 0
The draws below stay inside these ranges and needn't reach their ends.
There are 2 independent parts, one for each index of `grp`. The reference program is written for one: setup_inputs(seed, part) draws one part's arguments, and reference() takes and returns one part's arrays. A program takes and returns all parts, laid end to end along the dimension named above; an argument that names none is the same for every part. Nothing has to cross between parts.
Inputs may be any that keep to these rules, and one draw needn't show every extreme that they name: `token_count`: the number of real tokens of the complex; pair entries with either token index at or past it are padding.
All inputs are finite; a program needn't handle non-finite values.
Results may differ from the reference program's by a relative error of at most 0.015.
Values may be sent and summed in bfloat16 or wider, within the bound.
A program may use at most 64 MiB of HBM per device.

```python
import jax
import jax.numpy as jnp
from jax import lax

PAIR_DIM = 128
HIDDEN_SIZE = 128
FFN = 512
TOKENS = 384


def levels(own_key, shape, cuts, least, top_value):
    loudness = 1.0
    for position, parts in cuts:
        steps = jax.random.uniform(jax.random.fold_in(jax.random.fold_in(own_key, 6), position), (parts,), jnp.float32, least / len(cuts), top_value / len(cuts))
        loudness = loudness * jnp.repeat(jnp.exp(steps), shape[position] // parts).reshape((-1,) + (1,) * (len(shape) - 1 - position))
    return loudness


def normal_values(rng, extent, width, limit, split=(), held_as=jnp.bfloat16):
    gain = levels(rng, extent, split, -0.22, 0.18) if split else 1.0
    entries = jax.random.normal(rng, extent, jnp.float32) * width * gain
    return jnp.minimum(jnp.maximum(entries, -limit), limit).astype(held_as)


def setup_inputs(seed: int = 0, part: int = 0) -> dict:
    arg_keys = jax.random.split(jax.random.key(seed), 8)
    own_keys = jax.random.split(jax.random.fold_in(arg_keys[7], part), 8)
    pair = normal_values(own_keys[0], (TOKENS, TOKENS, PAIR_DIM), 1.0, 6.0, ((0, 32), (1, 4)))
    token_count = jax.random.randint(own_keys[1], (1,), 3 * TOKENS // 4, TOKENS + 1).astype(jnp.int32)
    tri_in = normal_values(arg_keys[2], (2, PAIR_DIM, 4 * HIDDEN_SIZE), PAIR_DIM ** -0.5, 0.5)
    tri_gate = normal_values(arg_keys[3], (2, PAIR_DIM, PAIR_DIM), PAIR_DIM ** -0.5, 0.5)
    tri_out = normal_values(arg_keys[4], (2, HIDDEN_SIZE, PAIR_DIM), HIDDEN_SIZE ** -0.5, 0.5)
    trans_in = normal_values(arg_keys[5], (PAIR_DIM, 2 * FFN), PAIR_DIM ** -0.5, 0.5)
    trans_out = normal_values(arg_keys[6], (FFN, PAIR_DIM), FFN ** -0.5, 0.25)
    return {"pair": pair, "token_count": token_count, "tri_in": tri_in, "tri_gate": tri_gate, "tri_out": tri_out, "trans_in": trans_in, "trans_out": trans_out}


def layer_norm(values, along):
    average = lax.optimization_barrier(jnp.mean(values, axis=along, keepdims=True))
    centred = values - average
    spread = lax.optimization_barrier(jnp.mean(centred * centred, axis=along, keepdims=True))
    return centred * lax.rsqrt(spread + 1e-05)

def rounded(values):
    return lax.optimization_barrier(values.astype(jnp.bfloat16)).astype(jnp.float32)

def triangle(stream, keep_mask, weight_in, weight_gate, weight_out, from_columns):
    hid_width = weight_out.shape[0]
    normed = rounded(layer_norm(stream.astype(jnp.float32), -1))
    projected = jnp.einsum('ijc,cd->ijd', normed, weight_in.astype(jnp.float32))
    keep_col = keep_mask[:, :, None]
    left_side = rounded(keep_col * jax.nn.sigmoid(projected[..., 2 * hid_width:3 * hid_width]) * projected[..., :hid_width])
    right_side = rounded(keep_col * jax.nn.sigmoid(projected[..., 3 * hid_width:]) * projected[..., hid_width:2 * hid_width])
    gate_value = jax.nn.sigmoid(jnp.einsum('ijc,cd->ijd', normed, weight_gate.astype(jnp.float32)))
    if from_columns:
        mixed_sum = jnp.einsum('kih,kjh->ijh', left_side, right_side)
    else:
        mixed_sum = jnp.einsum('ikh,jkh->ijh', left_side, right_side)
    mix_normed = rounded(layer_norm(mixed_sum, -1))
    update = gate_value * jnp.einsum('ijh,hc->ijc', mix_normed, weight_out.astype(jnp.float32))
    return (stream.astype(jnp.float32) + keep_col * update).astype(jnp.bfloat16)

def reference(pair, token_count, tri_in, tri_gate, tri_out, trans_in, trans_out):
    positions = jnp.arange(TOKENS, dtype=jnp.int32)
    is_valid = (positions < token_count[0]).astype(jnp.float32)
    keep_mask = is_valid[:, None] * is_valid[None, :]
    stream = triangle(pair, keep_mask, tri_in[0], tri_gate[0], tri_out[0], False)
    stream = triangle(stream, keep_mask, tri_in[1], tri_gate[1], tri_out[1], True)
    ffn_width = trans_out.shape[0]
    normed = rounded(layer_norm(stream.astype(jnp.float32), -1))
    inner_sum = jnp.einsum('ijc,cd->ijd', normed, trans_in.astype(jnp.float32))
    activation = rounded(jax.nn.silu(inner_sum[..., :ffn_width]) * inner_sum[..., ffn_width:])
    update = jnp.einsum('ijf,fc->ijc', activation, trans_out.astype(jnp.float32))
    return (stream.astype(jnp.float32) + keep_mask[:, :, None] * update).astype(jnp.bfloat16)
```

```python
import jax
import jax.numpy as jnp
from jax import lax
from jax.sharding import Mesh
from jax.sharding import PartitionSpec as P

ROW = ("row_0", "row_1")
GRP_ROW = ("grp", "row_0", "row_1")
NAMES = ("row_0", "row_1", "col")


def layer_norm(values, along):
    average = jnp.mean(values, axis=along, keepdims=True)
    centred = values - average
    spread = jnp.mean(centred * centred, axis=along, keepdims=True)
    return centred * lax.rsqrt(spread + 1e-05)


def exchange(blocks):
    return lax.all_to_all(blocks, NAMES, split_axis=0, concat_axis=0, tiled=True)


def body(pair, token_count, tri_in, tri_gate, tri_out, trans_in, trans_out):
    tile_rows, tile_cols, pair_width = pair.shape
    hidden = tri_out.shape[1]
    ffn_width = trans_out.shape[0]
    n_row = lax.axis_size("row_0") * lax.axis_size("row_1")
    n_col = lax.axis_size("col")
    row_place = lax.axis_index(ROW)
    col_place = lax.axis_index("col")
    token_limit = token_count[0]
    row_keep = (row_place * tile_rows + jnp.arange(tile_rows, dtype=jnp.int32) < token_limit).astype(jnp.float32)
    col_keep = (col_place * tile_cols + jnp.arange(tile_cols, dtype=jnp.int32) < token_limit).astype(jnp.float32)
    keep_mask = row_keep[:, None] * col_keep[None, :]
    tokens = n_row * tile_rows

    def triangle(stream, side):
        normed = layer_norm(stream.astype(jnp.float32), 2).astype(jnp.bfloat16)
        weight = tri_in[side].reshape(pair_width, 4, hidden)
        projected = jnp.einsum("ijc,cgh->ghij", normed, weight, preferred_element_type=jnp.float32)
        both = (keep_mask * jax.nn.sigmoid(projected[2:]) * projected[:2]).astype(jnp.bfloat16)
        gate_value = jax.nn.sigmoid(jnp.dot(normed, tri_gate[side], preferred_element_type=jnp.float32))
        got = exchange(both.transpose(1, 0, 2, 3))
        got = got.reshape(n_row, n_col, 2, tile_rows, tile_cols).transpose(2, 0, 3, 1, 4).reshape(2, tokens, tokens)
        if side == 0:
            mixed = lax.dot_general(got[0], got[1], (((1,), (1,)), ((), ())), preferred_element_type=jnp.float32)
        else:
            mixed = lax.dot_general(got[0], got[1], (((0,), (0,)), ((), ())), preferred_element_type=jnp.float32)
        mixed = mixed.astype(jnp.bfloat16).reshape(n_row, tile_rows, n_col, tile_cols).transpose(0, 2, 1, 3)
        back = exchange(mixed.reshape(n_row * n_col, tile_rows, tile_cols))
        mixnorm = layer_norm(back.astype(jnp.float32), 0).astype(jnp.bfloat16)
        update = gate_value * jnp.einsum("hij,hc->ijc", mixnorm, tri_out[side], preferred_element_type=jnp.float32)
        return (stream.astype(jnp.float32) + keep_mask[:, :, None] * update).astype(jnp.bfloat16)

    stream = triangle(pair, 0)
    stream = triangle(stream, 1)
    normed = layer_norm(stream.astype(jnp.float32), 2).astype(jnp.bfloat16)
    inner_sum = jnp.dot(normed, trans_in, preferred_element_type=jnp.float32)
    activation = (jax.nn.silu(inner_sum[..., :ffn_width]) * inner_sum[..., ffn_width:]).astype(jnp.bfloat16)
    update = jnp.dot(activation, trans_out, preferred_element_type=jnp.float32)
    return (stream.astype(jnp.float32) + keep_mask[:, :, None] * update).astype(jnp.bfloat16)


def solution(mesh):
    cores = 2
    torus = Mesh(
        mesh.devices.reshape(mesh.shape["grp"], mesh.shape["row"] // cores, cores, mesh.shape["col"]),
        ("grp", "row_0", "row_1", "col"),
    )
    placed = (P(GRP_ROW, "col", None), P("grp"), P(), P(), P(), P(), P())
    return jax.shard_map(body, mesh=torus, in_specs=placed, out_specs=P(GRP_ROW, "col", None), check_vma=False)
```

```python
import functools

import jax
import jax.numpy as jnp
from jax import lax
from jax.experimental import pallas as pl
from jax.experimental.pallas import tpu as pltpu
from jax.sharding import Mesh
from jax.sharding import PartitionSpec as P

MESH = pl.DeviceIdType.MESH
F32, BF16 = jnp.float32, jnp.bfloat16
CORES = 2


def log2(n):
    assert n & (n - 1) == 0
    return n.bit_length() - 1


def dot(a, b, ca, cb):
    return lax.dot_general(a, b, (((ca,), (cb,)), ((), ())), preferred_element_type=F32)


def layer_norm(v):
    average = jnp.mean(v, axis=0, keepdims=True)
    centred = v - average
    spread = jnp.mean(centred * centred, axis=0, keepdims=True)
    return centred * lax.rsqrt(spread + 1e-05)


def one_hot(shape, source_of_row):
    row = lax.broadcasted_iota(jnp.int32, shape, 0)
    col = lax.broadcasted_iota(jnp.int32, shape, 1)
    return (source_of_row(row) == col).astype(F32).astype(BF16)


def kernel(
    dims, count_ref, pair_ref, tri_in_ref, tri_gate_ref, tri_out_ref, trans_in_ref, trans_out_ref, out_ref,
    stream, normed, gate, keep, z_out, z_in, x_out, x_in, left, right, mixed,
    xb_out, xb_in, zb_out, zb_in, zs, zr, xs, xr, zbs, zbr, xbs, xbr,
):
    nz, nx, ti, tk = dims
    nc = CORES
    np_ = nc * nx
    tile, chan = pair_ref.shape
    hidden = tri_out_ref.shape[1]
    ffn = trans_out_ref.shape[0]
    size = nx * tk
    z, c, x = lax.axis_index("row_0"), lax.axis_index("row_1"), lax.axis_index("col")
    me = c * nx + x
    step = tile // 3
    pieces = [slice(k * step, (k + 1) * step) for k in range(3)]
    far_first = sorted(range(1, nz), key=lambda d: -min(d, nz - d))

    def z_peer(d):
        return lax.rem(z + d, nz)

    others = [(dc, dx) for dx in sorted(range(nx), key=lambda d: -min(d, nx - d)) for dc in range(nc) if dc or dx]

    def x_peer(o):
        return lax.rem(c + o[0], nc), lax.rem(x + o[1], nx)

    barrier = pltpu.get_barrier_semaphore()
    for d in far_first:
        pl.semaphore_signal(barrier, inc=1, device_id={"row_0": z_peer(d)}, device_id_type=MESH)
    for o in others:
        tc, tx = x_peer(o)
        pl.semaphore_signal(barrier, inc=1, device_id={"row_1": tc, "col": tx}, device_id_type=MESH)

    def z_exchange(source, target, ss, rs):
        copies = []
        for n, d in enumerate(far_first):
            t = z_peer(d)
            copy = pltpu.make_async_remote_copy(
                src_ref=source.at[t], dst_ref=target.at[z], send_sem=ss.at[n], recv_sem=rs.at[n],
                device_id={"row_0": t}, device_id_type=MESH,
            )
            copy.start()
            copies.append(copy)
        target[z] = source[z]
        return copies

    def x_exchange(source, target, ss, rs):
        copies = []
        for n, o in enumerate(others):
            tc, tx = x_peer(o)
            copy = pltpu.make_async_remote_copy(
                src_ref=source.at[tc * nx + tx], dst_ref=target.at[me], send_sem=ss.at[n], recv_sem=rs.at[n],
                device_id={"row_1": tc, "col": tx}, device_id_type=MESH,
            )
            copy.start()
            copies.append(copy)
        target[me] = source[me]
        return copies

    def finish(copies):
        for copy in copies:
            copy.wait()

    token = lax.broadcasted_iota(jnp.int32, (1, tile), 1)
    row = sum((token >= k * tk).astype(jnp.int32) for k in range(1, ti))
    limit = count_ref[0]
    inside = ((z * nc + c) * ti + row < limit) & (x * tk + token - row * tk < limit)
    keep[...] = jnp.where(inside, 1.0, 0.0).astype(F32)

    for piece in pieces:
        stream[:, piece] = pair_ref[piece, :].astype(F32).T.astype(BF16)

    lz, lp = log2(nz), log2(np_)

    for side in range(2):
        w_in = tri_in_ref[side]
        for piece in pieces:
            v = layer_norm(stream[:, piece].astype(F32)).astype(BF16)
            normed[:, piece] = v
            value = dot(w_in, v, 0, 0)
            both = keep[:, piece] * jax.nn.sigmoid(value[2 * hidden :]) * value[: 2 * hidden]
            both = both.astype(BF16)
            for k in range(nz):
                z_out[side, k, 0:np_, piece] = both[k * np_ : (k + 1) * np_]
                z_out[side, k, np_ : 2 * np_, piece] = both[hidden + k * np_ : hidden + (k + 1) * np_]
        if side == 0:
            pl.semaphore_wait(barrier, len(far_first) + len(others))
        copies = z_exchange(z_out.at[side], z_in.at[side], zs.at[side], zr.at[side])
        for piece in pieces:
            gate[:, piece] = jax.nn.sigmoid(dot(tri_gate_ref[side], normed[:, piece], 0, 0))
        n = 2 * hidden
        swap = one_hot((n, n), lambda r: ((r & (2 * nz - 1)) & (nz - 1)) * (2 * np_) + ((r >> lz) & 1) * np_ + (r >> (lz + 1)))
        finish(copies)
        for piece in pieces:
            got = z_in[side, :, :, piece].reshape(n, step)
            x_out[side, :, :, piece] = dot(swap, got, 1, 0).astype(BF16).reshape(np_, 2 * nz, step)
        copies = x_exchange(x_out.at[side], x_in.at[side], xs.at[side], xr.at[side])
        order = one_hot((size, size), lambda r: (r & (nz - 1)) * (nc * ti) + (r >> lz))
        finish(copies)
        for cc in range(nc):
            for i in range(ti):
                rows = slice((cc * ti + i) * nz, (cc * ti + i + 1) * nz)
                for xx in range(nx):
                    cols = slice(xx * tk, (xx + 1) * tk)
                    left[rows, cols] = x_in[side, cc * nx + xx, 0:nz, i * tk : (i + 1) * tk]
                    right[rows, cols] = x_in[side, cc * nx + xx, nz : 2 * nz, i * tk : (i + 1) * tk]
        if side == 0:
            product = dot(left[...], right[...], 1, 1).astype(BF16)
            mixed[...] = dot(product, order, 1, 0).astype(BF16)
        else:
            turned = dot(order, left[...], 1, 1).astype(BF16)
            mixed[...] = dot(turned, right[...], 1, 0).astype(BF16)
        for cc in range(nc):
            for i in range(ti):
                rows = slice((cc * ti + i) * nz, (cc * ti + i + 1) * nz)
                for xx in range(nx):
                    xb_out[side, cc * nx + xx, :, i * tk : (i + 1) * tk] = mixed[rows, xx * tk : (xx + 1) * tk]
        copies = x_exchange(xb_out.at[side], xb_in.at[side], xbs.at[side], xbr.at[side])
        swap = one_hot((hidden, hidden), lambda r: (r & (np_ - 1)) * nz + (r >> lp))
        finish(copies)
        for piece in pieces:
            got = xb_in[side, :, :, piece].reshape(hidden, step)
            zb_out[side, :, :, piece] = dot(swap, got, 1, 0).astype(BF16).reshape(nz, np_, step)
        copies = z_exchange(zb_out.at[side], zb_in.at[side], zbs.at[side], zbr.at[side])
        finish(copies)
        for piece in pieces:
            got = zb_in[side, :, :, piece].reshape(hidden, step)
            v = layer_norm(got.astype(F32)).astype(BF16)
            update = gate[:, piece] * dot(tri_out_ref[side], v, 0, 0)
            stream[:, piece] = (stream[:, piece].astype(F32) + keep[:, piece] * update).astype(BF16)

    for piece in pieces:
        base = stream[:, piece].astype(F32)
        v = layer_norm(base).astype(BF16)
        inner = dot(trans_in_ref[...], v, 0, 0)
        act = (jax.nn.silu(inner[:ffn]) * inner[ffn:]).astype(BF16)
        update = dot(trans_out_ref[...], act, 0, 0)
        out_ref[piece, :] = (base + keep[:, piece] * update).T.astype(BF16)


def body(pair, token_count, tri_in, tri_gate, tri_out, trans_in, trans_out):
    ti, tk, chan = pair.shape
    hidden = tri_out.shape[1]
    nz, nx = lax.axis_size("row_0"), lax.axis_size("col")
    np_ = CORES * nx
    tile, size = ti * tk, nx * tk
    vmem = pl.BlockSpec(memory_space=pltpu.VMEM)
    sem = pltpu.SemaphoreType.DMA
    out = pl.pallas_call(
        functools.partial(kernel, (nz, nx, ti, tk)),
        out_shape=jax.ShapeDtypeStruct((tile, chan), BF16),
        in_specs=[pl.BlockSpec(memory_space=pltpu.SMEM)] + [vmem] * 6,
        out_specs=vmem,
        scratch_shapes=[
            pltpu.VMEM((chan, tile), BF16),
            pltpu.VMEM((chan, tile), BF16),
            pltpu.VMEM((chan, tile), F32),
            pltpu.VMEM((1, tile), F32),
            pltpu.VMEM((2, nz, 2 * np_, tile), BF16),
            pltpu.VMEM((2, nz, 2 * np_, tile), BF16),
            pltpu.VMEM((2, np_, 2 * nz, tile), BF16),
            pltpu.VMEM((2, np_, 2 * nz, tile), BF16),
            pltpu.VMEM((size, size), BF16),
            pltpu.VMEM((size, size), BF16),
            pltpu.VMEM((size, size), BF16),
            pltpu.VMEM((2, np_, nz, tile), BF16),
            pltpu.VMEM((2, np_, nz, tile), BF16),
            pltpu.VMEM((2, nz, np_, tile), BF16),
            pltpu.VMEM((2, nz, np_, tile), BF16),
            sem((2, nz)), sem((2, nz)), sem((2, np_)), sem((2, np_)),
            sem((2, nz)), sem((2, nz)), sem((2, np_)), sem((2, np_)),
        ],
        compiler_params=pltpu.CompilerParams(
            collective_id=0, has_side_effects=True, vmem_limit_bytes=56 * 1024 * 1024
        ),
        name="pairformer_block",
    )(token_count, pair.reshape(tile, chan), tri_in, tri_gate, tri_out, trans_in, trans_out)
    return out.reshape(ti, tk, chan)


def solution(mesh):
    torus = Mesh(
        mesh.devices.reshape(mesh.shape["grp"], mesh.shape["row"] // CORES, CORES, mesh.shape["col"]),
        ("grp", "row_0", "row_1", "col"),
    )
    grp_row = ("grp", "row_0", "row_1")
    placed = (P(grp_row, "col", None), P("grp"), P(), P(), P(), P(), P())
    return jax.shard_map(
        body, mesh=torus, in_specs=placed, out_specs=P(grp_row, "col", None), check_vma=False
    )
```

```python
import functools

import jax
import jax.numpy as jnp
from jax import lax
from jax.experimental import pallas as pl
from jax.experimental.pallas import tpu as pltpu
from jax.sharding import Mesh
from jax.sharding import PartitionSpec as P

MESH = pl.DeviceIdType.MESH
F32, BF16 = jnp.float32, jnp.bfloat16
CORES = 2
PIECES = 3


def log2(n):
    assert n & (n - 1) == 0
    return n.bit_length() - 1


def dot(a, b, ca, cb):
    return lax.dot_general(a, b, (((ca,), (cb,)), ((), ())), preferred_element_type=F32)


def layer_norm(v):
    average = jnp.mean(v, axis=0, keepdims=True)
    centred = v - average
    spread = jnp.mean(centred * centred, axis=0, keepdims=True)
    return centred * lax.rsqrt(spread + 1e-05)


def one_hot(shape, source_of_row):
    row = lax.broadcasted_iota(jnp.int32, shape, 0)
    col = lax.broadcasted_iota(jnp.int32, shape, 1)
    return (source_of_row(row) == col).astype(F32).astype(BF16)


def kernel(
    dims, count_ref, pair_ref, tri_in_ref, tri_gate_ref, tri_out_ref, trans_in_ref, trans_out_ref, out_ref,
    stream, normed, gate, keep, left, right,
    w_out, w_in, y_out, y_in, yb_out, yb_in, wb_out, wb_in,
    ready, root_ready, zs, zr, xs, xr,
):
    nz, nx, ti, tk = dims
    nc = CORES
    np_ = nc * nx
    tile, chan = pair_ref.shape
    hidden = tri_out_ref.shape[1]
    ffn = trans_out_ref.shape[0]
    size = nx * tk
    z, c, x = lax.axis_index("row_0"), lax.axis_index("row_1"), lax.axis_index("col")
    me = c * nx + x
    step, ti_step = tile // PIECES, ti // PIECES
    pieces = [slice(k * step, (k + 1) * step) for k in range(PIECES)]
    whole = slice(0, tile)
    lz, lp = log2(nz), log2(np_)
    far_first = sorted(range(1, nz), key=lambda d: -min(d, nz - d))
    others = [(dc, dx) for dx in sorted(range(nx), key=lambda d: -min(d, nx - d)) for dc in range(nc) if dc or dx]

    def z_peer(d):
        return lax.rem(z + d, nz)

    def x_peer(o):
        return lax.rem(c + o[0], nc), lax.rem(x + o[1], nx)

    first_column = ((c == 0) & (x == 0)).astype(jnp.int32)
    place = lax.rem(z - first_column + nz, nz)
    last_comer = (z == 0) & (first_column == 1)
    barrier = pltpu.get_barrier_semaphore()

    def at_z(t):
        return {"row_0": t}

    def at_x(o):
        tc, tx = x_peer(o)
        return {"row_1": tc, "col": tx}

    @pl.when(jnp.logical_not(last_comer))
    def _():
        for o in others:
            pl.semaphore_signal(barrier, inc=1, device_id=at_x(o), device_id_type=MESH)

    greeted = len(others) - ((z == 0) & jnp.logical_not(last_comer)).astype(jnp.int32) + (place > 0).astype(jnp.int32)

    def enter():
        pl.semaphore_wait(barrier, greeted)

        @pl.when(place < nz - 1)
        def _():
            pl.semaphore_signal(barrier, inc=1, device_id=at_z(z_peer(1)), device_id_type=MESH)

        for d in range(1, nz):

            @pl.when(place >= d)
            def _():
                pl.semaphore_signal(ready.at[place], inc=1, device_id=at_z(z_peer(nz - d)), device_id_type=MESH)

        @pl.when(last_comer)
        def _():
            for o in others:
                pl.semaphore_signal(root_ready, inc=1, device_id=at_x(o), device_id_type=MESH)

    def all_entered():
        @pl.when((z == 0) & jnp.logical_not(last_comer))
        def _():
            pl.semaphore_wait(root_ready, 1)

    started = []
    used = {"z": 0, "x": 0}

    def bank_of(kind):
        used[kind] += 1
        return used[kind] - 1

    def all_bytes(ref, count, rows, lanes, sem):
        blocks = ref.at[0:count, rows, lanes]
        return pltpu.make_async_copy(blocks, blocks, sem)

    def z_copy(source, target, rows, lanes, bank, t):
        return pltpu.make_async_remote_copy(
            src_ref=source.at[t, rows, lanes], dst_ref=target.at[z, rows, lanes],
            send_sem=zs.at[bank], recv_sem=zr.at[bank], device_id=at_z(t), device_id_type=MESH,
        )

    def z_send(source, target, rows, lanes):
        bank = bank_of("z")
        for d in far_first:
            z_copy(source, target, rows, lanes, bank, z_peer(d)).start()
        target[z, rows, lanes] = source[z, rows, lanes]
        started.append(all_bytes(source, nz - 1, rows, lanes, zs.at[bank]))
        return all_bytes(target, nz - 1, rows, lanes, zr.at[bank])

    def z_send_as_they_enter(source, target, rows, lanes):
        bank = bank_of("z")
        for q in range(nz):

            @pl.when(q > place)
            def _():
                pl.semaphore_wait(ready.at[q], 1)

            @pl.when(q != place)
            def _():
                z_copy(source, target, rows, lanes, bank, lax.rem(q + first_column, nz)).start()

        target[z, rows, lanes] = source[z, rows, lanes]
        started.append(all_bytes(source, nz - 1, rows, lanes, zs.at[bank]))
        return all_bytes(target, nz - 1, rows, lanes, zr.at[bank])

    def x_send(source, target, rows, lanes):
        bank = bank_of("x")
        for o in others:
            tc, tx = x_peer(o)
            pltpu.make_async_remote_copy(
                src_ref=source.at[tc * nx + tx, rows, lanes], dst_ref=target.at[me, rows, lanes],
                send_sem=xs.at[bank], recv_sem=xr.at[bank], device_id=at_x(o), device_id_type=MESH,
            ).start()
        target[me, rows, lanes] = source[me, rows, lanes]
        started.append(all_bytes(source, np_ - 1, rows, lanes, xs.at[bank]))
        return all_bytes(target, np_ - 1, rows, lanes, xr.at[bank])

    def arrive(copies):
        copies.wait()

    token = lax.broadcasted_iota(jnp.int32, (1, tile), 1)
    row = sum((token >= k * tk).astype(jnp.int32) for k in range(1, ti))
    limit = count_ref[0]
    inside = ((z * nc + c) * ti + row < limit) & (x * tk + token - row * tk < limit)
    keep[...] = jnp.where(inside, 1.0, 0.0).astype(F32)

    def project(side, lanes, which):
        v = normed[:, lanes]
        cols = slice(which * hidden, (which + 1) * hidden)
        gates = slice((2 + which) * hidden, (3 + which) * hidden)
        value = dot(tri_in_ref[side, :, cols], v, 0, 0)
        opening = dot(tri_in_ref[side, :, gates], v, 0, 0)
        return (keep[:, lanes] * jax.nn.sigmoid(opening) * value).astype(BF16)

    def set_gate(side, lanes):
        gate[:, lanes] = jax.nn.sigmoid(dot(tri_gate_ref[side], normed[:, lanes], 0, 0))

    def update_stream(side, lanes):
        got = wb_in[side, :, :, lanes].reshape(hidden, step)
        v = layer_norm(got.astype(F32)).astype(BF16)
        update = gate[:, lanes] * dot(tri_out_ref[side], v, 0, 0)
        return (stream[:, lanes].astype(F32) + keep[:, lanes] * update).astype(BF16)

    to_x = one_hot((hidden, hidden), lambda r: (r & (nz - 1)) * np_ + (r >> lz))
    to_z = one_hot((hidden, hidden), lambda r: (r & (np_ - 1)) * nz + (r >> lp))
    order = one_hot((size, size), lambda r: (r & (nz - 1)) * (nc * ti) + (r >> lz))

    def z_to_x(side, which, lanes):
        got = w_in[side, :, which * np_ : (which + 1) * np_, lanes]
        got = got.reshape(hidden, got.shape[2])
        y_out[side, :, which * nz : (which + 1) * nz, lanes] = dot(to_x, got, 1, 0).astype(BF16).reshape(np_, nz, got.shape[1])

    def x_to_z(side, lanes):
        got = yb_in[side, :, :, lanes].reshape(hidden, step)
        wb_out[side, :, :, lanes] = dot(to_z, got, 1, 0).astype(BF16).reshape(nz, np_, step)

    def gather_rows(source, target, rows_of, first):
        for cc in range(nc):
            for i in rows_of:
                base = (cc * len(rows_of) + i - rows_of[0]) * nz
                for xx in range(nx):
                    target[base : base + nz, xx * tk : (xx + 1) * tk] = source[
                        cc * nx + xx, first : first + nz, i * tk : (i + 1) * tk
                    ]

    def spread_rows(value, target, rows_of, row_first, row_count):
        for cc in range(nc):
            for i in rows_of:
                base = (cc * row_count + i - row_first) * nz
                for xx in range(nx):
                    target[cc * nx + xx, :, i * tk : (i + 1) * tk] = value[base : base + nz, xx * tk : (xx + 1) * tk]

    rows_of = [list(range(k * ti_step, (k + 1) * ti_step)) for k in range(PIECES)]
    rows_all = list(range(ti))

    both, a_rows, b_rows = slice(0, 2 * np_), slice(0, nz), slice(nz, 2 * nz)

    def project_both(side, lanes):
        w_out[side, :, 0:np_, lanes] = project(side, lanes, 0).reshape(nz, np_, step)
        w_out[side, :, np_ : 2 * np_, lanes] = project(side, lanes, 1).reshape(nz, np_, step)

    def go_back(side, k, arrivals):
        arrive(arrivals)
        x_to_z(side, pieces[k])
        return z_send(wb_out.at[side], wb_in.at[side], slice(0, np_), pieces[k])

    for lanes in pieces:
        v = pair_ref[lanes, :].astype(F32).T
        stream[:, lanes] = v.astype(BF16)
        normed[:, lanes] = layer_norm(v).astype(BF16)
        project_both(0, lanes)
        set_gate(0, lanes)
    enter()
    here = z_send_as_they_enter(w_out.at[0], w_in.at[0], both, whole)
    all_entered()
    arrive(here)
    for lanes in pieces:
        z_to_x(0, 1, lanes)
    b_there = x_send(y_out.at[0], y_in.at[0], b_rows, whole)
    there = []
    for lanes in pieces:
        z_to_x(0, 0, lanes)
        there.append(x_send(y_out.at[0], y_in.at[0], a_rows, lanes))
    arrive(b_there)
    gather_rows(y_in.at[0], right, rows_all, nz)

    def multiply(k):
        arrive(there[k])
        gather_rows(y_in.at[0], left.at[k], rows_of[k], 0)
        product = dot(left[k], right[...], 1, 1).astype(BF16)
        value = dot(product, order, 1, 0).astype(BF16)
        spread_rows(value, yb_out.at[0], rows_of[k], rows_of[k][0], ti_step)
        return x_send(yb_out.at[0], yb_in.at[0], a_rows, pieces[k])

    mixed, home = [multiply(0)], []
    for k in range(PIECES):
        if k + 1 < PIECES:
            mixed.append(multiply(k + 1))
        home.append(go_back(0, k, mixed[k]))

    here = []
    for k, lanes in enumerate(pieces):
        arrive(home[k])
        v = update_stream(0, lanes)
        stream[:, lanes] = v
        normed[:, lanes] = layer_norm(v.astype(F32)).astype(BF16)
        project_both(1, lanes)
        here.append(z_send(w_out.at[1], w_in.at[1], both, lanes))
        set_gate(1, lanes)

    def forward(k):
        arrive(here[k])
        z_to_x(1, 0, pieces[k])
        z_to_x(1, 1, pieces[k])
        return x_send(y_out.at[1], y_in.at[1], slice(0, 2 * nz), pieces[k])

    count = ti_step * nc * nz

    def add(k, arrivals, so_far):
        arrive(arrivals)
        gather_rows(y_in.at[1], left.at[k], rows_of[k], 0)
        gather_rows(y_in.at[1], right.at[k * count : (k + 1) * count], rows_of[k], nz)
        turned = dot(order, left[k], 1, 1).astype(BF16)
        part = dot(turned, right[k * count : (k + 1) * count], 1, 0)
        return part if so_far is None else so_far + part

    there, sum_ = [forward(0)], None
    for k in range(PIECES):
        if k + 1 < PIECES:
            there.append(forward(k + 1))
        sum_ = add(k, there[k], sum_)
    value = sum_.astype(BF16)
    mixed = []
    for k in range(PIECES):
        spread_rows(value, yb_out.at[1], rows_of[k], 0, ti)
        mixed.append(x_send(yb_out.at[1], yb_in.at[1], a_rows, pieces[k]))
    home = [go_back(1, k, mixed[k]) for k in range(PIECES)]

    for k, lanes in enumerate(pieces):
        arrive(home[k])
        base = update_stream(1, lanes).astype(F32)
        v = layer_norm(base).astype(BF16)
        inner = dot(trans_in_ref[...], v, 0, 0)
        act = (jax.nn.silu(inner[:ffn]) * inner[ffn:]).astype(BF16)
        update = dot(trans_out_ref[...], act, 0, 0)
        out_ref[lanes, :] = (base + keep[:, lanes] * update).T.astype(BF16)

    for copies in started:
        copies.wait()


def body(pair, token_count, tri_in, tri_gate, tri_out, trans_in, trans_out):
    ti, tk, chan = pair.shape
    hidden = tri_out.shape[1]
    nz, nx = lax.axis_size("row_0"), lax.axis_size("col")
    np_ = CORES * nx
    tile, size = ti * tk, nx * tk
    vmem = pl.BlockSpec(memory_space=pltpu.VMEM)
    sem = pltpu.SemaphoreType.DMA

    def buffers(*shape):
        return [pltpu.VMEM(shape, BF16)] * 2

    z_banks, x_banks = 1 + 3 * PIECES, 1 + 4 * PIECES
    out = pl.pallas_call(
        functools.partial(kernel, (nz, nx, ti, tk)),
        out_shape=jax.ShapeDtypeStruct((tile, chan), BF16),
        in_specs=[pl.BlockSpec(memory_space=pltpu.SMEM)] + [vmem] * 6,
        out_specs=vmem,
        scratch_shapes=[
            pltpu.VMEM((chan, tile), BF16),
            pltpu.VMEM((chan, tile), BF16),
            pltpu.VMEM((chan, tile), F32),
            pltpu.VMEM((1, tile), F32),
            pltpu.VMEM((PIECES, size // PIECES, size), BF16),
            pltpu.VMEM((size, size), BF16),
            *buffers(2, nz, 2 * np_, tile),
            *buffers(2, np_, 2 * nz, tile),
            *buffers(2, np_, nz, tile),
            *buffers(2, nz, np_, tile),
            pltpu.SemaphoreType.REGULAR((nz,)), pltpu.SemaphoreType.REGULAR,
            sem((z_banks,)), sem((z_banks,)), sem((x_banks,)), sem((x_banks,)),
        ],
        compiler_params=pltpu.CompilerParams(
            collective_id=0, has_side_effects=True, vmem_limit_bytes=56 * 1024 * 1024
        ),
        name="pairformer_block",
    )(token_count, pair.reshape(tile, chan), tri_in, tri_gate, tri_out, trans_in, trans_out)
    return out.reshape(ti, tk, chan)


def solution(mesh):
    torus = Mesh(
        mesh.devices.reshape(mesh.shape["grp"], mesh.shape["row"] // CORES, CORES, mesh.shape["col"]),
        ("grp", "row_0", "row_1", "col"),
    )
    grp_row = ("grp", "row_0", "row_1")
    placed = (P(grp_row, "col", None), P("grp"), P(), P(), P(), P(), P())
    return jax.shard_map(
        body, mesh=torus, in_specs=placed, out_specs=P(grp_row, "col", None), check_vma=False
    )
```

```python
import functools

import jax
import jax.numpy as jnp
from jax import lax
from jax.experimental import pallas as pl
from jax.experimental.pallas import tpu as pltpu
from jax.sharding import Mesh
from jax.sharding import PartitionSpec as P

MESH = pl.DeviceIdType.MESH
F32, BF16 = jnp.float32, jnp.bfloat16
CORES = 2
PIECES = 3


def log2(n):
    assert n & (n - 1) == 0
    return n.bit_length() - 1


def dot(a, b, ca, cb):
    return lax.dot_general(a, b, (((ca,), (cb,)), ((), ())), preferred_element_type=F32)


def layer_norm(v):
    average = jnp.mean(v, axis=0, keepdims=True)
    centred = v - average
    spread = jnp.mean(centred * centred, axis=0, keepdims=True)
    return centred * lax.rsqrt(spread + 1e-05)


def one_hot(shape, source_of_row):
    row = lax.broadcasted_iota(jnp.int32, shape, 0)
    col = lax.broadcasted_iota(jnp.int32, shape, 1)
    return (source_of_row(row) == col).astype(F32).astype(BF16)


def kernel(
    dims, count_ref, pair_ref, tri_in_ref, tri_gate_ref, tri_out_ref, trans_in_ref, trans_out_ref, out_ref,
    stream, stream_c, normed, normed_c, gate, keep, left, right, turned, right_c,
    w_out, w_in, y_out, y_in, yb_out, yb_in, wb_out, wb_in,
    zs, zr, xs, xr,
):
    nz, nx, ti, tk = dims
    nc = CORES
    np_ = nc * nx
    tile, chan = pair_ref.shape
    hidden = tri_out_ref.shape[1]
    ffn = trans_out_ref.shape[0]
    size = nx * tk
    z, c, x = lax.axis_index("row_0"), lax.axis_index("row_1"), lax.axis_index("col")
    me = c * nx + x
    step, ti_step, part = tile // PIECES, ti // PIECES, tk // PIECES
    count = ti_step * nc * nz
    pieces = [slice(k * step, (k + 1) * step) for k in range(PIECES)]
    whole = slice(0, tile)
    lz, lp = log2(nz), log2(np_)
    far_first = sorted(range(1, nz), key=lambda d: -min(d, nz - d))
    others = [(dc, dx) for dx in sorted(range(nx), key=lambda d: -min(d, nx - d)) for dc in range(nc) if dc or dx]

    def z_peer(d):
        return lax.rem(z + d, nz)

    def x_peer(o):
        return lax.rem(c + o[0], nc), lax.rem(x + o[1], nx)

    def at_z(t):
        return {"row_0": t}

    def at_x(o):
        tc, tx = x_peer(o)
        return {"row_1": tc, "col": tx}

    barrier = pltpu.get_barrier_semaphore()
    for d in far_first:
        pl.semaphore_signal(barrier, inc=1, device_id=at_z(z_peer(d)), device_id_type=MESH)
    for o in others:
        pl.semaphore_signal(barrier, inc=1, device_id=at_x(o), device_id_type=MESH)

    started = []
    used = {"z": 0, "x": 0}

    def bank_of(kind):
        used[kind] += 1
        return used[kind] - 1

    def all_bytes(ref, count, rows, lanes, sem):
        blocks = ref.at[0:count, rows, lanes]
        return pltpu.make_async_copy(blocks, blocks, sem)

    def z_copy(source, target, rows, lanes, bank, t):
        return pltpu.make_async_remote_copy(
            src_ref=source.at[t, rows, lanes], dst_ref=target.at[z, rows, lanes],
            send_sem=zs.at[bank], recv_sem=zr.at[bank], device_id=at_z(t), device_id_type=MESH,
        )

    def z_send(source, target, rows, lanes):
        bank = bank_of("z")
        for d in far_first:
            z_copy(source, target, rows, lanes, bank, z_peer(d)).start()
        target[z, rows, lanes] = source[z, rows, lanes]
        started.append(all_bytes(source, nz - 1, rows, lanes, zs.at[bank]))
        return all_bytes(target, nz - 1, rows, lanes, zr.at[bank])

    def x_send(source, target, rows, lanes):
        bank = bank_of("x")
        for o in others:
            tc, tx = x_peer(o)
            pltpu.make_async_remote_copy(
                src_ref=source.at[tc * nx + tx, rows, lanes], dst_ref=target.at[me, rows, lanes],
                send_sem=xs.at[bank], recv_sem=xr.at[bank], device_id=at_x(o), device_id_type=MESH,
            ).start()
        target[me, rows, lanes] = source[me, rows, lanes]
        started.append(all_bytes(source, np_ - 1, rows, lanes, xs.at[bank]))
        return all_bytes(target, np_ - 1, rows, lanes, xr.at[bank])

    def arrive(copies):
        copies.wait()

    token = lax.broadcasted_iota(jnp.int32, (1, tile), 1)
    limit = count_ref[0]

    def inside(row, col):
        valid = ((z * nc + c) * ti + row < limit) & (x * tk + col < limit)
        return jnp.where(valid, 1.0, 0.0).astype(F32)

    def count_steps(value, length, most):
        return sum((value >= m * length).astype(jnp.int32) for m in range(1, most))

    by_row = count_steps(token, tk, ti)
    keep[0:1] = inside(by_row, token - by_row * tk)
    piece = count_steps(token, step, PIECES)
    rest = token - piece * step
    by_row = count_steps(rest, part, ti)
    keep[1:2] = inside(by_row, piece * part + rest - by_row * part)

    def by_columns(source, target, rows_of_piece):
        for i in rows_of_piece:
            for q in range(PIECES):
                at = q * step + i * part
                target[:, at : at + part] = source[:, i * tk + q * part : i * tk + (q + 1) * part]

    def project(side, lanes, which, source, mask):
        v = source[:, lanes]
        cols = slice(which * hidden, (which + 1) * hidden)
        gates = slice((2 + which) * hidden, (3 + which) * hidden)
        value = dot(tri_in_ref[side, :, cols], v, 0, 0)
        opening = dot(tri_in_ref[side, :, gates], v, 0, 0)
        value = (keep[mask : mask + 1, lanes] * jax.nn.sigmoid(opening) * value).astype(BF16)
        w_out[side, :, which * np_ : (which + 1) * np_, lanes] = value.reshape(nz, np_, step)

    def set_gate(side, lanes, source):
        gate[:, lanes] = jax.nn.sigmoid(dot(tri_gate_ref[side], source[:, lanes], 0, 0))

    def update_stream(side, lanes, source):
        got = wb_in[side, :, :, lanes].reshape(hidden, step)
        v = layer_norm(got.astype(F32)).astype(BF16)
        update = gate[:, lanes] * dot(tri_out_ref[side], v, 0, 0)
        return (source[:, lanes].astype(F32) + keep[side : side + 1, lanes] * update).astype(BF16)

    to_x = one_hot((hidden, hidden), lambda r: (r & (nz - 1)) * np_ + (r >> lz))
    to_z = one_hot((hidden, hidden), lambda r: (r & (np_ - 1)) * nz + (r >> lp))
    order = one_hot((size, size), lambda r: (r & (nz - 1)) * (nc * ti) + (r >> lz))

    def z_to_x(side, which, lanes):
        got = w_in[side, :, which * np_ : (which + 1) * np_, lanes]
        got = got.reshape(hidden, got.shape[2])
        y_out[side, :, which * nz : (which + 1) * nz, lanes] = dot(to_x, got, 1, 0).astype(BF16).reshape(np_, nz, got.shape[1])

    def x_to_z(side, lanes):
        got = yb_in[side, :, :, lanes].reshape(hidden, step)
        wb_out[side, :, :, lanes] = dot(to_z, got, 1, 0).astype(BF16).reshape(nz, np_, step)

    def gather_rows(source, target, rows_of, rows, lane, width):
        for cc in range(nc):
            for i in rows_of:
                base = (cc * len(rows_of) + i - rows_of[0]) * nz
                at = lane + i * width
                for xx in range(nx):
                    target[base : base + nz, xx * width : (xx + 1) * width] = source[cc * nx + xx, rows, at : at + width]

    def spread_rows(value, target, rows_of, lane, width):
        for cc in range(nc):
            for i in rows_of:
                base = (cc * len(rows_of) + i - rows_of[0]) * nz
                at = lane + i * width
                for xx in range(nx):
                    target[cc * nx + xx, :, at : at + width] = value[base : base + nz, xx * width : (xx + 1) * width]

    rows_of = [list(range(k * ti_step, (k + 1) * ti_step)) for k in range(PIECES)]
    rows_all = list(range(ti))

    a_in, b_in = slice(0, np_), slice(np_, 2 * np_)
    a_rows, b_rows = slice(0, nz), slice(nz, 2 * nz)

    def send_w(side, rows, lanes):
        return z_send(w_out.at[side], w_in.at[side], rows, lanes)

    def forward(side, which, lanes, arrivals):
        arrive(arrivals)
        z_to_x(side, which, lanes)
        return x_send(y_out.at[side], y_in.at[side], (a_rows, b_rows)[which], lanes)

    def go_back(side, k, arrivals):
        arrive(arrivals)
        x_to_z(side, pieces[k])
        return z_send(wb_out.at[side], wb_in.at[side], slice(0, np_), pieces[k])

    for lanes in pieces:
        v = pair_ref[lanes, :].astype(F32).T
        stream[:, lanes] = v.astype(BF16)
        normed[:, lanes] = layer_norm(v).astype(BF16)
        project(0, lanes, 1, normed, 0)
    for lanes in pieces:
        project(0, lanes, 0, normed, 0)
    pl.semaphore_wait(barrier, len(far_first) + len(others))
    b_here = send_w(0, b_in, whole)
    a_here = [send_w(0, a_in, lanes) for lanes in pieces]
    for lanes in pieces:
        set_gate(0, lanes, normed)
    arrive(b_here)
    for lanes in pieces:
        z_to_x(0, 1, lanes)
    b_there = x_send(y_out.at[0], y_in.at[0], b_rows, whole)
    there = [forward(0, 0, pieces[0], a_here[0])]
    arrive(b_there)
    gather_rows(y_in.at[0], right, rows_all, b_rows, 0, tk)

    def multiply(k):
        arrive(there[k])
        gather_rows(y_in.at[0], left.at[k * count : (k + 1) * count], rows_of[k], a_rows, 0, tk)
        product = dot(left[k * count : (k + 1) * count], right[...], 1, 1).astype(BF16)
        value = dot(product, order, 1, 0).astype(BF16)
        spread_rows(value, yb_out.at[0], rows_of[k], 0, tk)
        return x_send(yb_out.at[0], yb_in.at[0], a_rows, pieces[k])

    mixed, home = [], []
    for k in range(PIECES):
        mixed.append(multiply(k))
        if k + 1 < PIECES:
            there.append(forward(0, 0, pieces[k + 1], a_here[k + 1]))
        if k > 0:
            home.append(go_back(0, k - 1, mixed[k - 1]))
    home.append(go_back(0, PIECES - 1, mixed[PIECES - 1]))

    a_here = []
    for k, lanes in enumerate(pieces):
        arrive(home[k])
        v = update_stream(0, lanes, stream)
        stream[:, lanes] = v
        normed[:, lanes] = layer_norm(v.astype(F32)).astype(BF16)
        project(1, lanes, 0, normed, 0)
        a_here.append(send_w(1, a_in, lanes))
        by_columns(normed, normed_c, rows_of[k])
    b_here = []
    for lanes in pieces:
        project(1, lanes, 1, normed_c, 1)
        b_here.append(send_w(1, b_in, lanes))
    by_columns(stream, stream_c, rows_all)
    for lanes in pieces:
        set_gate(1, lanes, normed_c)
    there = [forward(1, 0, pieces[k], a_here[k]) for k in range(PIECES)]
    for k in range(PIECES):
        arrive(there[k])
        gather_rows(y_in.at[1], left.at[k * count : (k + 1) * count], rows_of[k], a_rows, 0, tk)
        turned[:, k * count : (k + 1) * count] = dot(order, left[k * count : (k + 1) * count], 1, 1).astype(BF16)
    there = [forward(1, 1, pieces[0], b_here[0])]

    def multiply(q):
        arrive(there[q])
        for k in range(PIECES):
            gather_rows(y_in.at[1], right_c.at[q, k * count : (k + 1) * count], rows_of[k], b_rows, q * step, part)
        value = dot(turned[...], right_c[q], 1, 0).astype(BF16)
        spread_rows(value, yb_out.at[1], rows_all, q * step, part)
        return x_send(yb_out.at[1], yb_in.at[1], a_rows, pieces[q])

    mixed, home = [], []
    for q in range(PIECES):
        mixed.append(multiply(q))
        if q + 1 < PIECES:
            there.append(forward(1, 1, pieces[q + 1], b_here[q + 1]))
        if q > 0:
            home.append(go_back(1, q - 1, mixed[q - 1]))
    home.append(go_back(1, PIECES - 1, mixed[PIECES - 1]))

    for q, lanes in enumerate(pieces):
        arrive(home[q])
        base = update_stream(1, lanes, stream_c).astype(F32)
        v = layer_norm(base).astype(BF16)
        inner = dot(trans_in_ref[...], v, 0, 0)
        act = (jax.nn.silu(inner[:ffn]) * inner[ffn:]).astype(BF16)
        update = dot(trans_out_ref[...], act, 0, 0)
        result = (base + keep[1:2, lanes] * update).T.astype(BF16)
        for i in range(ti):
            out_ref[i * tk + q * part : i * tk + (q + 1) * part, :] = result[i * part : (i + 1) * part]

    for copies in started:
        copies.wait()


def body(pair, token_count, tri_in, tri_gate, tri_out, trans_in, trans_out):
    ti, tk, chan = pair.shape
    hidden = tri_out.shape[1]
    nz, nx = lax.axis_size("row_0"), lax.axis_size("col")
    np_ = CORES * nx
    tile, size = ti * tk, nx * tk
    vmem = pl.BlockSpec(memory_space=pltpu.VMEM)
    sem = pltpu.SemaphoreType.DMA

    def buffers(*shape):
        return [pltpu.VMEM(shape, BF16)] * 2

    z_banks, x_banks = 1 + 5 * PIECES, 1 + 5 * PIECES
    out = pl.pallas_call(
        functools.partial(kernel, (nz, nx, ti, tk)),
        out_shape=jax.ShapeDtypeStruct((tile, chan), BF16),
        in_specs=[pl.BlockSpec(memory_space=pltpu.SMEM)] + [vmem] * 6,
        out_specs=vmem,
        scratch_shapes=[
            *buffers(chan, tile),
            *buffers(chan, tile),
            pltpu.VMEM((chan, tile), F32),
            pltpu.VMEM((2, tile), F32),
            *buffers(size, size),
            pltpu.VMEM((size, size), BF16),
            pltpu.VMEM((PIECES, size, size // PIECES), BF16),
            *buffers(2, nz, 2 * np_, tile),
            *buffers(2, np_, 2 * nz, tile),
            *buffers(2, np_, nz, tile),
            *buffers(2, nz, np_, tile),
            sem((z_banks,)), sem((z_banks,)), sem((x_banks,)), sem((x_banks,)),
        ],
        compiler_params=pltpu.CompilerParams(
            collective_id=0, has_side_effects=True, vmem_limit_bytes=56 * 1024 * 1024
        ),
        name="pairformer_block",
    )(token_count, pair.reshape(tile, chan), tri_in, tri_gate, tri_out, trans_in, trans_out)
    return out.reshape(ti, tk, chan)


def solution(mesh):
    torus = Mesh(
        mesh.devices.reshape(mesh.shape["grp"], mesh.shape["row"] // CORES, CORES, mesh.shape["col"]),
        ("grp", "row_0", "row_1", "col"),
    )
    grp_row = ("grp", "row_0", "row_1")
    placed = (P(grp_row, "col", None), P("grp"), P(), P(), P(), P(), P())
    return jax.shard_map(
        body, mesh=torus, in_specs=placed, out_specs=P(grp_row, "col", None), check_vma=False
    )
```

```python
import functools

import jax
import jax.numpy as jnp
from jax import lax
from jax.experimental import pallas as pl
from jax.experimental.pallas import tpu as pltpu
from jax.sharding import Mesh
from jax.sharding import PartitionSpec as P

MESH = pl.DeviceIdType.MESH
F32, BF16 = jnp.float32, jnp.bfloat16
CORES = 2
PIECES = 3


def log2(n):
    assert n & (n - 1) == 0
    return n.bit_length() - 1


def dot(a, b, ca, cb):
    return lax.dot_general(a, b, (((ca,), (cb,)), ((), ())), preferred_element_type=F32)


def layer_norm(v):
    average = jnp.mean(v, axis=0, keepdims=True)
    centred = v - average
    spread = jnp.mean(centred * centred, axis=0, keepdims=True)
    return centred * lax.rsqrt(spread + 1e-05)


def one_hot(shape, source_of_row):
    row = lax.broadcasted_iota(jnp.int32, shape, 0)
    col = lax.broadcasted_iota(jnp.int32, shape, 1)
    return (source_of_row(row) == col).astype(F32).astype(BF16)


def kernel(
    dims, count_ref, pair_ref, tri_in_ref, tri_gate_ref, tri_out_ref, trans_in_ref, trans_out_ref, out_ref,
    stream, stream_c, normed, normed_c, gate, keep, left, right, turned, right_c,
    w_out, w_in, y_out, y_in, yb_out, yb_in, wb_out, wb_in,
    zs, zr, xs, xr,
):
    nz, nx, ti, tk = dims
    nc = CORES
    np_ = nc * nx
    tile, chan = pair_ref.shape
    hidden = tri_out_ref.shape[1]
    ffn = trans_out_ref.shape[0]
    size = nx * tk
    z, c, x = lax.axis_index("row_0"), lax.axis_index("row_1"), lax.axis_index("col")
    me = c * nx + x
    step, ti_step, part = tile // PIECES, ti // PIECES, tk // PIECES
    count = ti_step * nc * nz
    pieces = [slice(k * step, (k + 1) * step) for k in range(PIECES)]
    whole = slice(0, tile)
    lz, lp = log2(nz), log2(np_)
    far_first = sorted(range(1, nz), key=lambda d: -min(d, nz - d))
    others = [(dc, dx) for dx in sorted(range(nx), key=lambda d: -min(d, nx - d)) for dc in range(nc) if dc or dx]

    def z_peer(d):
        return lax.rem(z + d, nz)

    def x_peer(o):
        return lax.rem(c + o[0], nc), lax.rem(x + o[1], nx)

    def at_z(t):
        return {"row_0": t}

    def at_x(o):
        tc, tx = x_peer(o)
        return {"row_1": tc, "col": tx}

    barrier = pltpu.get_barrier_semaphore()
    for d in far_first:
        pl.semaphore_signal(barrier, inc=1, device_id=at_z(z_peer(d)), device_id_type=MESH)
    for o in others:
        pl.semaphore_signal(barrier, inc=1, device_id=at_x(o), device_id_type=MESH)

    started = []
    used = {"z": 0, "x": 0}

    def bank_of(kind):
        used[kind] += 1
        return used[kind] - 1

    def all_bytes(ref, count, rows, lanes, sem):
        blocks = ref.at[0:count, rows, lanes]
        return pltpu.make_async_copy(blocks, blocks, sem)

    def z_copy(source, target, rows, lanes, bank, t):
        return pltpu.make_async_remote_copy(
            src_ref=source.at[t, rows, lanes], dst_ref=target.at[z, rows, lanes],
            send_sem=zs.at[bank], recv_sem=zr.at[bank], device_id=at_z(t), device_id_type=MESH,
        )

    def z_send(source, target, rows, lanes):
        bank = bank_of("z")
        for d in far_first:
            z_copy(source, target, rows, lanes, bank, z_peer(d)).start()
        target[z, rows, lanes] = source[z, rows, lanes]
        started.append(all_bytes(source, nz - 1, rows, lanes, zs.at[bank]))
        return all_bytes(target, nz - 1, rows, lanes, zr.at[bank])

    def x_send(source, target, rows, lanes):
        bank = bank_of("x")
        for o in others:
            tc, tx = x_peer(o)
            pltpu.make_async_remote_copy(
                src_ref=source.at[tc * nx + tx, rows, lanes], dst_ref=target.at[me, rows, lanes],
                send_sem=xs.at[bank], recv_sem=xr.at[bank], device_id=at_x(o), device_id_type=MESH,
            ).start()
        target[me, rows, lanes] = source[me, rows, lanes]
        started.append(all_bytes(source, np_ - 1, rows, lanes, xs.at[bank]))
        return all_bytes(target, np_ - 1, rows, lanes, xr.at[bank])

    def arrive(copies):
        copies.wait()

    token = lax.broadcasted_iota(jnp.int32, (1, tile), 1)
    limit = count_ref[0]

    def inside(row, col):
        valid = ((z * nc + c) * ti + row < limit) & (x * tk + col < limit)
        return jnp.where(valid, 1.0, 0.0).astype(F32)

    def count_steps(value, length, most):
        return sum((value >= m * length).astype(jnp.int32) for m in range(1, most))

    by_row = count_steps(token, tk, ti)
    keep[0:1] = inside(by_row, token - by_row * tk)
    piece = count_steps(token, step, PIECES)
    rest = token - piece * step
    by_row = count_steps(rest, part, ti)
    keep[1:2] = inside(by_row, piece * part + rest - by_row * part)

    def by_columns(source, target, rows_of_piece):
        for i in rows_of_piece:
            for q in range(PIECES):
                at = q * step + i * part
                target[:, at : at + part] = source[:, i * tk + q * part : i * tk + (q + 1) * part]

    def project(side, lanes, which, source, mask):
        v = source[:, lanes]
        cols = slice(which * hidden, (which + 1) * hidden)
        gates = slice((2 + which) * hidden, (3 + which) * hidden)
        value = dot(tri_in_ref[side, :, cols], v, 0, 0)
        opening = dot(tri_in_ref[side, :, gates], v, 0, 0)
        value = (keep[mask : mask + 1, lanes] * jax.nn.sigmoid(opening) * value).astype(BF16)
        w_out[side, :, which * np_ : (which + 1) * np_, lanes] = value.reshape(nz, np_, step)

    def set_gate(side, lanes, source):
        gate[:, lanes] = jax.nn.sigmoid(dot(tri_gate_ref[side], source[:, lanes], 0, 0))

    def update_stream(side, lanes, source):
        got = wb_in[side, :, :, lanes].reshape(hidden, step)
        v = layer_norm(got.astype(F32)).astype(BF16)
        update = gate[:, lanes] * dot(tri_out_ref[side], v, 0, 0)
        return (source[:, lanes].astype(F32) + keep[side : side + 1, lanes] * update).astype(BF16)

    to_x = one_hot((hidden, hidden), lambda r: (r & (nz - 1)) * np_ + (r >> lz))
    to_z = one_hot((hidden, hidden), lambda r: (r & (np_ - 1)) * nz + (r >> lp))
    order = one_hot((size, size), lambda r: (r & (nz - 1)) * (nc * ti) + (r >> lz))

    def z_to_x(side, which, lanes):
        got = w_in[side, :, which * np_ : (which + 1) * np_, lanes]
        got = got.reshape(hidden, got.shape[2])
        y_out[side, :, which * nz : (which + 1) * nz, lanes] = dot(to_x, got, 1, 0).astype(BF16).reshape(np_, nz, got.shape[1])

    def x_to_z(side, lanes):
        got = yb_in[side, :, :, lanes].reshape(hidden, step)
        wb_out[side, :, :, lanes] = dot(to_z, got, 1, 0).astype(BF16).reshape(nz, np_, step)

    def gather_rows(source, target, rows_of, rows, lane, width):
        for cc in range(nc):
            for i in rows_of:
                base = (cc * len(rows_of) + i - rows_of[0]) * nz
                at = lane + i * width
                for xx in range(nx):
                    target[base : base + nz, xx * width : (xx + 1) * width] = source[cc * nx + xx, rows, at : at + width]

    def spread_rows(value, target, rows_of, lane, width):
        for cc in range(nc):
            for i in rows_of:
                base = (cc * len(rows_of) + i - rows_of[0]) * nz
                at = lane + i * width
                for xx in range(nx):
                    target[cc * nx + xx, :, at : at + width] = value[base : base + nz, xx * width : (xx + 1) * width]

    rows_of = [list(range(k * ti_step, (k + 1) * ti_step)) for k in range(PIECES)]
    rows_all = list(range(ti))

    a_in, b_in = slice(0, np_), slice(np_, 2 * np_)
    a_rows, b_rows = slice(0, nz), slice(nz, 2 * nz)

    def send_w(side, rows, lanes):
        return z_send(w_out.at[side], w_in.at[side], rows, lanes)

    def forward(side, which, lanes, arrivals):
        arrive(arrivals)
        z_to_x(side, which, lanes)
        return x_send(y_out.at[side], y_in.at[side], (a_rows, b_rows)[which], lanes)

    def go_back(side, k, arrivals):
        arrive(arrivals)
        x_to_z(side, pieces[k])
        return z_send(wb_out.at[side], wb_in.at[side], slice(0, np_), pieces[k])

    def in_steps(forth, product, back, first):
        there, mixed, home = {0: first}, {}, {}
        there[1] = forth(1)
        for k in range(PIECES):
            mixed[k] = product(k, there[k])
            if k + 2 < PIECES:
                there[k + 2] = forth(k + 2)
            if k > 0:
                home[k - 1] = back(k - 1, mixed[k - 1])
        home[PIECES - 1] = back(PIECES - 1, mixed[PIECES - 1])
        return [home[k] for k in range(PIECES)]

    b_here, a_here = [], []
    for k, lanes in enumerate(pieces):
        v = pair_ref[lanes, :].astype(F32).T
        stream[:, lanes] = v.astype(BF16)
        normed[:, lanes] = layer_norm(v).astype(BF16)
        project(0, lanes, 1, normed, 0)
        if k == 0:
            pl.semaphore_wait(barrier, len(far_first) + len(others))
        b_here.append(send_w(0, b_in, lanes))
    for lanes in pieces:
        project(0, lanes, 0, normed, 0)
        a_here.append(send_w(0, a_in, lanes))
    for lanes in pieces:
        set_gate(0, lanes, normed)
    for lanes, arrivals in zip(pieces, b_here):
        arrive(arrivals)
        z_to_x(0, 1, lanes)
    b_there = x_send(y_out.at[0], y_in.at[0], b_rows, whole)
    there = [forward(0, 0, pieces[0], a_here[0])]
    arrive(b_there)
    gather_rows(y_in.at[0], right, rows_all, b_rows, 0, tk)

    def multiply(k, arrivals):
        arrive(arrivals)
        gather_rows(y_in.at[0], left.at[k * count : (k + 1) * count], rows_of[k], a_rows, 0, tk)
        product = dot(left[k * count : (k + 1) * count], right[...], 1, 1).astype(BF16)
        value = dot(product, order, 1, 0).astype(BF16)
        spread_rows(value, yb_out.at[0], rows_of[k], 0, tk)
        return x_send(yb_out.at[0], yb_in.at[0], a_rows, pieces[k])

    def forward_a(k):
        return forward(0, 0, pieces[k], a_here[k])

    home = in_steps(forward_a, multiply, lambda k, arrivals: go_back(0, k, arrivals), there[0])

    a_here = []
    for k, lanes in enumerate(pieces):
        arrive(home[k])
        v = update_stream(0, lanes, stream)
        stream[:, lanes] = v
        normed[:, lanes] = layer_norm(v.astype(F32)).astype(BF16)
        project(1, lanes, 0, normed, 0)
        a_here.append(send_w(1, a_in, lanes))
        by_columns(normed, normed_c, rows_of[k])
    b_here = []
    for lanes in pieces:
        project(1, lanes, 1, normed_c, 1)
        b_here.append(send_w(1, b_in, lanes))
    by_columns(stream, stream_c, rows_all)
    for lanes in pieces:
        set_gate(1, lanes, normed_c)
    there = [forward(1, 0, pieces[k], a_here[k]) for k in range(PIECES)]
    for k in range(PIECES):
        arrive(there[k])
        gather_rows(y_in.at[1], left.at[k * count : (k + 1) * count], rows_of[k], a_rows, 0, tk)
        turned[:, k * count : (k + 1) * count] = dot(order, left[k * count : (k + 1) * count], 1, 1).astype(BF16)
    there = [forward(1, 1, pieces[0], b_here[0])]

    def multiply(q, arrivals):
        arrive(arrivals)
        for k in range(PIECES):
            gather_rows(y_in.at[1], right_c.at[q, k * count : (k + 1) * count], rows_of[k], b_rows, q * step, part)
        value = dot(turned[...], right_c[q], 1, 0).astype(BF16)
        spread_rows(value, yb_out.at[1], rows_all, q * step, part)
        return x_send(yb_out.at[1], yb_in.at[1], a_rows, pieces[q])

    def forward_b(q):
        return forward(1, 1, pieces[q], b_here[q])

    home = in_steps(forward_b, multiply, lambda q, arrivals: go_back(1, q, arrivals), there[0])

    for q, lanes in enumerate(pieces):
        arrive(home[q])
        base = update_stream(1, lanes, stream_c).astype(F32)
        v = layer_norm(base).astype(BF16)
        inner = dot(trans_in_ref[...], v, 0, 0)
        act = (jax.nn.silu(inner[:ffn]) * inner[ffn:]).astype(BF16)
        update = dot(trans_out_ref[...], act, 0, 0)
        result = (base + keep[1:2, lanes] * update).T.astype(BF16)
        for i in range(ti):
            out_ref[i * tk + q * part : i * tk + (q + 1) * part, :] = result[i * part : (i + 1) * part]

    for copies in started:
        copies.wait()


def body(pair, token_count, tri_in, tri_gate, tri_out, trans_in, trans_out):
    ti, tk, chan = pair.shape
    hidden = tri_out.shape[1]
    nz, nx = lax.axis_size("row_0"), lax.axis_size("col")
    np_ = CORES * nx
    tile, size = ti * tk, nx * tk
    vmem = pl.BlockSpec(memory_space=pltpu.VMEM)
    sem = pltpu.SemaphoreType.DMA

    def buffers(*shape):
        return [pltpu.VMEM(shape, BF16)] * 2

    z_banks, x_banks = 6 * PIECES, 1 + 5 * PIECES
    out = pl.pallas_call(
        functools.partial(kernel, (nz, nx, ti, tk)),
        out_shape=jax.ShapeDtypeStruct((tile, chan), BF16),
        in_specs=[pl.BlockSpec(memory_space=pltpu.SMEM)] + [vmem] * 6,
        out_specs=vmem,
        scratch_shapes=[
            *buffers(chan, tile),
            *buffers(chan, tile),
            pltpu.VMEM((chan, tile), F32),
            pltpu.VMEM((2, tile), F32),
            *buffers(size, size),
            pltpu.VMEM((size, size), BF16),
            pltpu.VMEM((PIECES, size, size // PIECES), BF16),
            *buffers(2, nz, 2 * np_, tile),
            *buffers(2, np_, 2 * nz, tile),
            *buffers(2, np_, nz, tile),
            *buffers(2, nz, np_, tile),
            sem((z_banks,)), sem((z_banks,)), sem((x_banks,)), sem((x_banks,)),
        ],
        compiler_params=pltpu.CompilerParams(
            collective_id=0, has_side_effects=True, vmem_limit_bytes=56 * 1024 * 1024
        ),
        name="pairformer_block",
    )(token_count, pair.reshape(tile, chan), tri_in, tri_gate, tri_out, trans_in, trans_out)
    return out.reshape(ti, tk, chan)


def solution(mesh):
    torus = Mesh(
        mesh.devices.reshape(mesh.shape["grp"], mesh.shape["row"] // CORES, CORES, mesh.shape["col"]),
        ("grp", "row_0", "row_1", "col"),
    )
    grp_row = ("grp", "row_0", "row_1")
    placed = (P(grp_row, "col", None), P("grp"), P(), P(), P(), P(), P())
    return jax.shard_map(
        body, mesh=torus, in_specs=placed, out_specs=P(grp_row, "col", None), check_vma=False
    )
```

```python
import functools

import jax
import jax.numpy as jnp
from jax import lax
from jax.experimental import pallas as pl
from jax.experimental.pallas import tpu as pltpu
from jax.sharding import Mesh
from jax.sharding import PartitionSpec as P

MESH = pl.DeviceIdType.MESH
F32, BF16 = jnp.float32, jnp.bfloat16
CORES = 2
PIECES = 3


def log2(n):
    assert n & (n - 1) == 0
    return n.bit_length() - 1


def dot(a, b, ca, cb):
    return lax.dot_general(a, b, (((ca,), (cb,)), ((), ())), preferred_element_type=F32)


def layer_norm(v):
    average = jnp.mean(v, axis=0, keepdims=True)
    centred = v - average
    spread = jnp.mean(centred * centred, axis=0, keepdims=True)
    return centred * lax.rsqrt(spread + 1e-05)


def one_hot(shape, source_of_row):
    row = lax.broadcasted_iota(jnp.int32, shape, 0)
    col = lax.broadcasted_iota(jnp.int32, shape, 1)
    return (source_of_row(row) == col).astype(F32).astype(BF16)


def kernel(
    dims, count_ref, pair_ref, tri_in_ref, tri_gate_ref, tri_out_ref, trans_in_ref, trans_out_ref, out_ref,
    stream, stream_c, normed, normed_c, gate, keep, left, right, turned, right_c,
    w_out, w_in, y_out, y_in, yb_out, yb_in, wb_out, wb_in, zc_out, zc_in,
    zs, zr, xs, xr,
):
    nz, nx, ti, tk = dims
    nc = CORES
    np_ = nc * nx
    tile, chan = pair_ref.shape
    hidden = tri_out_ref.shape[1]
    ffn = trans_out_ref.shape[0]
    size = nx * tk
    z, c, x = lax.axis_index("row_0"), lax.axis_index("row_1"), lax.axis_index("col")
    me = c * nx + x
    step, ti_step, part = tile // PIECES, ti // PIECES, tk // PIECES
    count = ti_step * nc * nz
    pieces = [slice(k * step, (k + 1) * step) for k in range(PIECES)]
    whole = slice(0, tile)
    lz, lp = log2(nz), log2(np_)
    far_first = sorted(range(1, nz), key=lambda d: -min(d, nz - d))
    others = [(dc, dx) for dx in sorted(range(nx), key=lambda d: -min(d, nx - d)) for dc in range(nc) if dc or dx]

    def z_peer(d):
        return lax.rem(z + d, nz)

    def x_peer(o):
        return lax.rem(c + o[0], nc), lax.rem(x + o[1], nx)

    def at_z(t):
        return {"row_0": t}

    def at_x(o):
        tc, tx = x_peer(o)
        return {"row_1": tc, "col": tx}

    barrier = pltpu.get_barrier_semaphore()
    for d in far_first:
        pl.semaphore_signal(barrier, inc=1, device_id=at_z(z_peer(d)), device_id_type=MESH)
    for o in others:
        pl.semaphore_signal(barrier, inc=1, device_id=at_x(o), device_id_type=MESH)

    started = []
    used = {"z": 0, "x": 0}

    def bank_of(kind):
        used[kind] += 1
        return used[kind] - 1

    def all_bytes(ref, count, rows, lanes, sem):
        blocks = ref.at[0:count, rows, lanes]
        return pltpu.make_async_copy(blocks, blocks, sem)

    def z_copy(source, target, rows, lanes, bank, t):
        return pltpu.make_async_remote_copy(
            src_ref=source.at[t, rows, lanes], dst_ref=target.at[z, rows, lanes],
            send_sem=zs.at[bank], recv_sem=zr.at[bank], device_id=at_z(t), device_id_type=MESH,
        )

    def z_send(source, target, rows, lanes):
        bank = bank_of("z")
        for d in far_first:
            z_copy(source, target, rows, lanes, bank, z_peer(d)).start()
        target[z, rows, lanes] = source[z, rows, lanes]
        started.append(all_bytes(source, nz - 1, rows, lanes, zs.at[bank]))
        return all_bytes(target, nz - 1, rows, lanes, zr.at[bank])

    def x_send(source, target, rows, lanes):
        bank = bank_of("x")
        for o in others:
            tc, tx = x_peer(o)
            pltpu.make_async_remote_copy(
                src_ref=source.at[tc * nx + tx, rows, lanes], dst_ref=target.at[me, rows, lanes],
                send_sem=xs.at[bank], recv_sem=xr.at[bank], device_id=at_x(o), device_id_type=MESH,
            ).start()
        target[me, rows, lanes] = source[me, rows, lanes]
        started.append(all_bytes(source, np_ - 1, rows, lanes, xs.at[bank]))
        return all_bytes(target, np_ - 1, rows, lanes, xr.at[bank])

    def arrive(copies):
        copies.wait()

    token = lax.broadcasted_iota(jnp.int32, (1, tile), 1)
    limit = count_ref[0]

    def inside(row, col):
        valid = ((z * nc + c) * ti + row < limit) & (x * tk + col < limit)
        return jnp.where(valid, 1.0, 0.0).astype(F32)

    def count_steps(value, length, most):
        return sum((value >= m * length).astype(jnp.int32) for m in range(1, most))

    by_row = count_steps(token, tk, ti)
    keep[0:1] = inside(by_row, token - by_row * tk)
    piece = count_steps(token, step, PIECES)
    rest = token - piece * step
    by_row = count_steps(rest, part, ti)
    keep[1:2] = inside(by_row, piece * part + rest - by_row * part)

    def by_columns(source, target, rows_of_piece):
        for i in rows_of_piece:
            for q in range(PIECES):
                at = q * step + i * part
                target[:, at : at + part] = source[:, i * tk + q * part : i * tk + (q + 1) * part]

    def project(side, lanes, which, source, mask):
        v = source[:, lanes]
        cols = slice(which * hidden, (which + 1) * hidden)
        gates = slice((2 + which) * hidden, (3 + which) * hidden)
        value = dot(tri_in_ref[side, :, cols], v, 0, 0)
        opening = dot(tri_in_ref[side, :, gates], v, 0, 0)
        value = (keep[mask : mask + 1, lanes] * jax.nn.sigmoid(opening) * value).astype(BF16)
        w_out[side, :, which * np_ : (which + 1) * np_, lanes] = value.reshape(nz, np_, step)

    def set_gate(side, lanes, source):
        gate[:, lanes] = jax.nn.sigmoid(dot(tri_gate_ref[side], source[:, lanes], 0, 0))

    def update_stream(side, lanes, source, arrived, weights):
        got = arrived[:, :, lanes].reshape(hidden, step)
        v = layer_norm(got.astype(F32)).astype(BF16)
        update = gate[:, lanes] * dot(weights, v, 0, 0)
        return (source[:, lanes].astype(F32) + keep[side : side + 1, lanes] * update).astype(BF16)

    def z_to_x(side, which, lanes):
        got = w_in[side, :, which * np_ : (which + 1) * np_, lanes]
        got = got.reshape(hidden, got.shape[2])
        y_out[side, :, which * nz : (which + 1) * nz, lanes] = dot(to_x, got, 1, 0).astype(BF16).reshape(np_, nz, got.shape[1])

    def x_to_z(lanes):
        got = yb_in[1, :, :, lanes].reshape(hidden, step)
        wb_out[:, :, lanes] = dot(to_z, got, 1, 0).astype(BF16).reshape(nz, np_, step)

    def gather_rows(source, target, rows_of, rows, lane, width):
        for cc in range(nc):
            for i in rows_of:
                base = (cc * len(rows_of) + i - rows_of[0]) * nz
                at = lane + i * width
                for xx in range(nx):
                    target[base : base + nz, xx * width : (xx + 1) * width] = source[cc * nx + xx, rows, at : at + width]

    def spread_rows(value, target, rows_of, lane, width):
        for cc in range(nc):
            for i in rows_of:
                base = (cc * len(rows_of) + i - rows_of[0]) * nz
                at = lane + i * width
                for xx in range(nx):
                    target[cc * nx + xx, :, at : at + width] = value[base : base + nz, xx * width : (xx + 1) * width]

    rows_of = [list(range(k * ti_step, (k + 1) * ti_step)) for k in range(PIECES)]
    rows_all = list(range(ti))

    a_in, b_in = slice(0, np_), slice(np_, 2 * np_)
    a_rows, b_rows = slice(0, nz), slice(nz, 2 * nz)

    def send_w(side, rows, lanes):
        return z_send(w_out.at[side], w_in.at[side], rows, lanes)

    def forward(side, which, lanes, arrivals):
        arrive(arrivals)
        z_to_x(side, which, lanes)
        return x_send(y_out.at[side], y_in.at[side], (a_rows, b_rows)[which], lanes)

    def go_back(k, arrivals):
        arrive(arrivals)
        x_to_z(pieces[k])
        return z_send(wb_out, wb_in, a_in, pieces[k])

    def in_steps(forth, product, back, first):
        there, mixed, home = {0: first}, {}, {}
        there[1] = forth(1)
        for k in range(PIECES):
            mixed[k] = product(k, there[k])
            if k + 2 < PIECES:
                there[k + 2] = forth(k + 2)
            if k > 0:
                home[k - 1] = back(k - 1, mixed[k - 1])
        home[PIECES - 1] = back(PIECES - 1, mixed[PIECES - 1])
        return [home[k] for k in range(PIECES)]

    b_here, a_here = [], []
    for k, lanes in enumerate(pieces):
        v = pair_ref[lanes, :].astype(F32).T
        stream[:, lanes] = v.astype(BF16)
        normed[:, lanes] = layer_norm(v).astype(BF16)
        project(0, lanes, 1, normed, 0)
        if k == 0:
            pl.semaphore_wait(barrier, len(far_first) + len(others))
        b_here.append(send_w(0, b_in, lanes))
    for lanes in pieces:
        project(0, lanes, 0, normed, 0)
        a_here.append(send_w(0, a_in, lanes))
    to_x = one_hot((hidden, hidden), lambda r: (r & (nz - 1)) * np_ + (r >> lz))
    to_z = one_hot((hidden, hidden), lambda r: (r & (np_ - 1)) * nz + (r >> lp))
    order = one_hot((size, size), lambda r: (r & (nz - 1)) * (nc * ti) + (r >> lz))
    row_places = nc * ti_step
    by_z = one_hot((count, count), lambda r: (r & (row_places - 1)) * nz + (r >> log2(row_places)))
    by_row = one_hot((count, count), lambda r: (r & (nz - 1)) * row_places + (r >> lz))
    out_weights = dot(to_x, tri_out_ref[0], 1, 0).astype(BF16)
    for lanes in pieces:
        set_gate(0, lanes, normed)
    for lanes, arrivals in zip(pieces, b_here):
        arrive(arrivals)
        z_to_x(0, 1, lanes)
    b_there = x_send(y_out.at[0], y_in.at[0], b_rows, whole)
    there = [forward(0, 0, pieces[0], a_here[0])]
    arrive(b_there)
    gather_rows(y_in.at[0], right, rows_all, b_rows, 0, tk)

    def multiply(k, arrivals):
        arrive(arrivals)
        gather_rows(y_in.at[0], left.at[k * count : (k + 1) * count], rows_of[k], a_rows, 0, tk)
        product = dot(left[k * count : (k + 1) * count], right[...], 1, 1).astype(BF16)
        value = dot(product, order, 1, 0).astype(BF16)
        zc_out[k] = dot(by_z, value, 1, 0).astype(BF16).reshape(nz, row_places, size)
        return z_send(zc_out.at[k], zc_in.at[k], slice(0, row_places), slice(0, size))

    def turn(k, arrivals):
        arrive(arrivals)
        value = dot(by_row, zc_in[k].reshape(count, size), 1, 0).astype(BF16)
        spread_rows(value, yb_out.at[0], rows_of[k], 0, tk)
        return x_send(yb_out.at[0], yb_in.at[0], a_rows, pieces[k])

    there.append(forward(0, 0, pieces[1], a_here[1]))
    mixed = []
    for k in range(PIECES):
        mixed.append(multiply(k, there[k]))
        if k + 2 < PIECES:
            there.append(forward(0, 0, pieces[k + 2], a_here[k + 2]))

    a_here, home = [], [turn(0, mixed[0])]
    for k, lanes in enumerate(pieces):
        if k + 1 < PIECES:
            home.append(turn(k + 1, mixed[k + 1]))
        arrive(home[k])
        v = update_stream(0, lanes, stream, yb_in.at[0], out_weights)
        stream[:, lanes] = v
        normed[:, lanes] = layer_norm(v.astype(F32)).astype(BF16)
        project(1, lanes, 0, normed, 0)
        a_here.append(send_w(1, a_in, lanes))
        by_columns(normed, normed_c, rows_of[k])
    b_here = []
    for lanes in pieces:
        project(1, lanes, 1, normed_c, 1)
        b_here.append(send_w(1, b_in, lanes))
    by_columns(stream, stream_c, rows_all)
    for lanes in pieces:
        set_gate(1, lanes, normed_c)
    there = [forward(1, 0, pieces[k], a_here[k]) for k in range(PIECES)]
    for k in range(PIECES):
        arrive(there[k])
        gather_rows(y_in.at[1], left.at[k * count : (k + 1) * count], rows_of[k], a_rows, 0, tk)
        turned[:, k * count : (k + 1) * count] = dot(order, left[k * count : (k + 1) * count], 1, 1).astype(BF16)
    there = [forward(1, 1, pieces[0], b_here[0])]

    def multiply(q, arrivals):
        arrive(arrivals)
        for k in range(PIECES):
            gather_rows(y_in.at[1], right_c.at[q, k * count : (k + 1) * count], rows_of[k], b_rows, q * step, part)
        value = dot(turned[...], right_c[q], 1, 0).astype(BF16)
        spread_rows(value, yb_out.at[1], rows_all, q * step, part)
        return x_send(yb_out.at[1], yb_in.at[1], a_rows, pieces[q])

    def forward_b(q):
        return forward(1, 1, pieces[q], b_here[q])

    home = in_steps(forward_b, multiply, go_back, there[0])

    for q, lanes in enumerate(pieces):
        arrive(home[q])
        base = update_stream(1, lanes, stream_c, wb_in, tri_out_ref[1]).astype(F32)
        v = layer_norm(base).astype(BF16)
        inner = dot(trans_in_ref[...], v, 0, 0)
        act = (jax.nn.silu(inner[:ffn]) * inner[ffn:]).astype(BF16)
        update = dot(trans_out_ref[...], act, 0, 0)
        result = (base + keep[1:2, lanes] * update).T.astype(BF16)
        for i in range(ti):
            out_ref[i * tk + q * part : i * tk + (q + 1) * part, :] = result[i * part : (i + 1) * part]

    for copies in started:
        copies.wait()


def body(pair, token_count, tri_in, tri_gate, tri_out, trans_in, trans_out):
    ti, tk, chan = pair.shape
    hidden = tri_out.shape[1]
    nz, nx = lax.axis_size("row_0"), lax.axis_size("col")
    np_ = CORES * nx
    tile, size = ti * tk, nx * tk
    vmem = pl.BlockSpec(memory_space=pltpu.VMEM)
    sem = pltpu.SemaphoreType.DMA

    def buffers(*shape):
        return [pltpu.VMEM(shape, BF16)] * 2

    z_banks, x_banks = 6 * PIECES, 1 + 5 * PIECES
    out = pl.pallas_call(
        functools.partial(kernel, (nz, nx, ti, tk)),
        out_shape=jax.ShapeDtypeStruct((tile, chan), BF16),
        in_specs=[pl.BlockSpec(memory_space=pltpu.SMEM)] + [vmem] * 6,
        out_specs=vmem,
        scratch_shapes=[
            *buffers(chan, tile),
            *buffers(chan, tile),
            pltpu.VMEM((chan, tile), F32),
            pltpu.VMEM((2, tile), F32),
            *buffers(size, size),
            pltpu.VMEM((size, size), BF16),
            pltpu.VMEM((PIECES, size, size // PIECES), BF16),
            *buffers(2, nz, 2 * np_, tile),
            *buffers(2, np_, 2 * nz, tile),
            *buffers(2, np_, nz, tile),
            *buffers(nz, np_, tile),
            *buffers(PIECES, nz, size // PIECES // nz, size),
            sem((z_banks,)), sem((z_banks,)), sem((x_banks,)), sem((x_banks,)),
        ],
        compiler_params=pltpu.CompilerParams(
            collective_id=0, has_side_effects=True, vmem_limit_bytes=56 * 1024 * 1024
        ),
        name="pairformer_block",
    )(token_count, pair.reshape(tile, chan), tri_in, tri_gate, tri_out, trans_in, trans_out)
    return out.reshape(ti, tk, chan)


def solution(mesh):
    torus = Mesh(
        mesh.devices.reshape(mesh.shape["grp"], mesh.shape["row"] // CORES, CORES, mesh.shape["col"]),
        ("grp", "row_0", "row_1", "col"),
    )
    grp_row = ("grp", "row_0", "row_1")
    placed = (P(grp_row, "col", None), P("grp"), P(), P(), P(), P(), P())
    return jax.shard_map(
        body, mesh=torus, in_specs=placed, out_specs=P(grp_row, "col", None), check_vma=False
    )
```

```python
import functools

import jax
import jax.numpy as jnp
from jax import lax
from jax.experimental import pallas as pl
from jax.experimental.pallas import tpu as pltpu
from jax.sharding import Mesh
from jax.sharding import PartitionSpec as P

MESH = pl.DeviceIdType.MESH
F32, BF16 = jnp.float32, jnp.bfloat16
CORES = 2
PIECES = 3


def log2(n):
    assert n & (n - 1) == 0
    return n.bit_length() - 1


def dot(a, b, ca, cb):
    return lax.dot_general(a, b, (((ca,), (cb,)), ((), ())), preferred_element_type=F32)


def layer_norm(v):
    average = jnp.mean(v, axis=0, keepdims=True)
    centred = v - average
    spread = jnp.mean(centred * centred, axis=0, keepdims=True)
    return centred * lax.rsqrt(spread + 1e-05)


def one_hot(shape, source_of_row):
    row = lax.broadcasted_iota(jnp.int32, shape, 0)
    col = lax.broadcasted_iota(jnp.int32, shape, 1)
    return (source_of_row(row) == col).astype(F32).astype(BF16)


def kernel(
    dims, count_ref, pair_hbm, tri_in_hbm, tri_gate_hbm, tri_out_hbm, trans_in_hbm, trans_out_hbm, out_hbm,
    out_ref, stores,
    pair_ref, tri_in_ref, tri_gate_ref, tri_out_ref, trans_in_ref, trans_out_ref, loads,
    stream, stream_c, normed, normed_c, gate, keep, left, right, turned, right_c,
    w_out, w_in, y_out, y_in, yb_out, yb_in, wb_out, wb_in, zc_out, zc_in,
    zs, zr, xs, xr,
):
    nz, nx, ti, tk = dims
    nc = CORES
    np_ = nc * nx
    tile, chan = pair_hbm.shape
    hidden = tri_out_hbm.shape[1]
    ffn = trans_out_hbm.shape[0]
    size = nx * tk
    z, c, x = lax.axis_index("row_0"), lax.axis_index("row_1"), lax.axis_index("col")
    me = c * nx + x
    step, ti_step, part = tile // PIECES, ti // PIECES, tk // PIECES
    count = ti_step * nc * nz
    pieces = [slice(k * step, (k + 1) * step) for k in range(PIECES)]
    whole = slice(0, tile)
    lz, lp = log2(nz), log2(np_)
    far_first = sorted(range(1, nz), key=lambda d: -min(d, nz - d))
    others = [(dc, dx) for dx in sorted(range(nx), key=lambda d: -min(d, nx - d)) for dc in range(nc) if dc or dx]

    def z_peer(d):
        return lax.rem(z + d, nz)

    def x_peer(o):
        return lax.rem(c + o[0], nc), lax.rem(x + o[1], nx)

    def at_z(t):
        return {"row_0": t}

    def at_x(o):
        tc, tx = x_peer(o)
        return {"row_1": tc, "col": tx}

    barrier = pltpu.get_barrier_semaphore()
    for d in far_first:
        pl.semaphore_signal(barrier, inc=1, device_id=at_z(z_peer(d)), device_id_type=MESH)
    for o in others:
        pl.semaphore_signal(barrier, inc=1, device_id=at_x(o), device_id_type=MESH)

    sources = (pair_hbm, tri_in_hbm, tri_gate_hbm, tri_out_hbm, trans_in_hbm, trans_out_hbm)
    targets = (pair_ref, tri_in_ref, tri_gate_ref, tri_out_ref, trans_in_ref, trans_out_ref)
    loading = [pltpu.make_async_copy(a, b, loads.at[n]) for n, (a, b) in enumerate(zip(sources, targets))]
    for copies in loading:
        copies.start()

    started = []
    used = {"z": 0, "x": 0}

    def bank_of(kind):
        used[kind] += 1
        return used[kind] - 1

    def all_bytes(ref, count, rows, lanes, sem):
        blocks = ref.at[0:count, rows, lanes]
        return pltpu.make_async_copy(blocks, blocks, sem)

    def z_copy(source, target, rows, lanes, bank, t):
        return pltpu.make_async_remote_copy(
            src_ref=source.at[t, rows, lanes], dst_ref=target.at[z, rows, lanes],
            send_sem=zs.at[bank], recv_sem=zr.at[bank], device_id=at_z(t), device_id_type=MESH,
        )

    def z_send(source, target, rows, lanes):
        bank = bank_of("z")
        for d in far_first:
            z_copy(source, target, rows, lanes, bank, z_peer(d)).start()
        target[z, rows, lanes] = source[z, rows, lanes]
        started.append(all_bytes(source, nz - 1, rows, lanes, zs.at[bank]))
        return all_bytes(target, nz - 1, rows, lanes, zr.at[bank])

    def x_send(source, target, rows, lanes):
        bank = bank_of("x")
        for o in others:
            tc, tx = x_peer(o)
            pltpu.make_async_remote_copy(
                src_ref=source.at[tc * nx + tx, rows, lanes], dst_ref=target.at[me, rows, lanes],
                send_sem=xs.at[bank], recv_sem=xr.at[bank], device_id=at_x(o), device_id_type=MESH,
            ).start()
        target[me, rows, lanes] = source[me, rows, lanes]
        started.append(all_bytes(source, np_ - 1, rows, lanes, xs.at[bank]))
        return all_bytes(target, np_ - 1, rows, lanes, xr.at[bank])

    def arrive(copies):
        copies.wait()

    token = lax.broadcasted_iota(jnp.int32, (1, tile), 1)
    limit = count_ref[0]

    def inside(row, col):
        valid = ((z * nc + c) * ti + row < limit) & (x * tk + col < limit)
        return jnp.where(valid, 1.0, 0.0).astype(F32)

    def count_steps(value, length, most):
        return sum((value >= m * length).astype(jnp.int32) for m in range(1, most))

    by_row = count_steps(token, tk, ti)
    keep[0:1] = inside(by_row, token - by_row * tk)
    piece = count_steps(token, step, PIECES)
    rest = token - piece * step
    by_row = count_steps(rest, part, ti)
    keep[1:2] = inside(by_row, piece * part + rest - by_row * part)

    def by_columns(source, target, rows_of_piece):
        for i in rows_of_piece:
            for q in range(PIECES):
                at = q * step + i * part
                target[:, at : at + part] = source[:, i * tk + q * part : i * tk + (q + 1) * part]

    def project(side, lanes, which, source, mask):
        v = source[:, lanes]
        cols = slice(which * hidden, (which + 1) * hidden)
        gates = slice((2 + which) * hidden, (3 + which) * hidden)
        value = dot(tri_in_ref[side, :, cols], v, 0, 0)
        opening = dot(tri_in_ref[side, :, gates], v, 0, 0)
        value = (keep[mask : mask + 1, lanes] * jax.nn.sigmoid(opening) * value).astype(BF16)
        w_out[side, :, which * np_ : (which + 1) * np_, lanes] = value.reshape(nz, np_, step)

    def set_gate(side, lanes, source):
        gate[:, lanes] = jax.nn.sigmoid(dot(tri_gate_ref[side], source[:, lanes], 0, 0))

    def update_stream(side, lanes, source, arrived, weights):
        got = arrived[:, :, lanes].reshape(hidden, step)
        v = layer_norm(got.astype(F32)).astype(BF16)
        update = gate[:, lanes] * dot(weights, v, 0, 0)
        return (source[:, lanes].astype(F32) + keep[side : side + 1, lanes] * update).astype(BF16)

    def z_to_x(side, which, lanes):
        got = w_in[side, :, which * np_ : (which + 1) * np_, lanes]
        got = got.reshape(hidden, got.shape[2])
        y_out[side, :, which * nz : (which + 1) * nz, lanes] = dot(to_x, got, 1, 0).astype(BF16).reshape(np_, nz, got.shape[1])

    def x_to_z(lanes):
        got = yb_in[1, :, :, lanes].reshape(hidden, step)
        wb_out[:, :, lanes] = dot(to_z, got, 1, 0).astype(BF16).reshape(nz, np_, step)

    def gather_rows(source, target, rows_of, rows, lane, width):
        for cc in range(nc):
            for i in rows_of:
                base = (cc * len(rows_of) + i - rows_of[0]) * nz
                at = lane + i * width
                for xx in range(nx):
                    target[base : base + nz, xx * width : (xx + 1) * width] = source[cc * nx + xx, rows, at : at + width]

    def spread_rows(value, target, rows_of, lane, width):
        for cc in range(nc):
            for i in rows_of:
                base = (cc * len(rows_of) + i - rows_of[0]) * nz
                at = lane + i * width
                for xx in range(nx):
                    target[cc * nx + xx, :, at : at + width] = value[base : base + nz, xx * width : (xx + 1) * width]

    rows_of = [list(range(k * ti_step, (k + 1) * ti_step)) for k in range(PIECES)]
    rows_all = list(range(ti))

    a_in, b_in = slice(0, np_), slice(np_, 2 * np_)
    a_rows, b_rows = slice(0, nz), slice(nz, 2 * nz)

    def send_w(side, rows, lanes):
        return z_send(w_out.at[side], w_in.at[side], rows, lanes)

    def forward(side, which, lanes, arrivals):
        arrive(arrivals)
        z_to_x(side, which, lanes)
        return x_send(y_out.at[side], y_in.at[side], (a_rows, b_rows)[which], lanes)

    def go_back(k, arrivals):
        arrive(arrivals)
        x_to_z(pieces[k])
        return z_send(wb_out, wb_in, a_in, pieces[k])

    def in_steps(forth, product, back, first):
        there, mixed, home = {0: first}, {}, {}
        there[1] = forth(1)
        for k in range(PIECES):
            mixed[k] = product(k, there[k])
            if k + 2 < PIECES:
                there[k + 2] = forth(k + 2)
            if k > 0:
                home[k - 1] = back(k - 1, mixed[k - 1])
        home[PIECES - 1] = back(PIECES - 1, mixed[PIECES - 1])
        return [home[k] for k in range(PIECES)]

    b_here, a_here = [], []
    loading[0].wait()
    loading[1].wait()
    for k, lanes in enumerate(pieces):
        v = pair_ref[lanes, :].astype(F32).T
        stream[:, lanes] = v.astype(BF16)
        normed[:, lanes] = layer_norm(v).astype(BF16)
        project(0, lanes, 1, normed, 0)
        if k == 0:
            pl.semaphore_wait(barrier, len(far_first) + len(others))
        b_here.append(send_w(0, b_in, lanes))
    for lanes in pieces:
        project(0, lanes, 0, normed, 0)
        a_here.append(send_w(0, a_in, lanes))
    for copies in loading[2:]:
        copies.wait()

    to_x = one_hot((hidden, hidden), lambda r: (r & (nz - 1)) * np_ + (r >> lz))
    to_z = one_hot((hidden, hidden), lambda r: (r & (np_ - 1)) * nz + (r >> lp))
    order = one_hot((size, size), lambda r: (r & (nz - 1)) * (nc * ti) + (r >> lz))
    row_places = nc * ti_step
    by_z = one_hot((count, count), lambda r: (r & (row_places - 1)) * nz + (r >> log2(row_places)))
    by_row = one_hot((count, count), lambda r: (r & (nz - 1)) * row_places + (r >> lz))
    out_weights = dot(to_x, tri_out_ref[0], 1, 0).astype(BF16)
    for lanes in pieces:
        set_gate(0, lanes, normed)
    for lanes, arrivals in zip(pieces, b_here):
        arrive(arrivals)
        z_to_x(0, 1, lanes)
    b_there = x_send(y_out.at[0], y_in.at[0], b_rows, whole)
    there = [forward(0, 0, pieces[0], a_here[0])]
    arrive(b_there)
    gather_rows(y_in.at[0], right, rows_all, b_rows, 0, tk)

    def multiply(k, arrivals):
        arrive(arrivals)
        gather_rows(y_in.at[0], left.at[k * count : (k + 1) * count], rows_of[k], a_rows, 0, tk)
        product = dot(left[k * count : (k + 1) * count], right[...], 1, 1).astype(BF16)
        value = dot(product, order, 1, 0).astype(BF16)
        zc_out[k] = dot(by_z, value, 1, 0).astype(BF16).reshape(nz, row_places, size)
        return z_send(zc_out.at[k], zc_in.at[k], slice(0, row_places), slice(0, size))

    def turn(k, arrivals):
        arrive(arrivals)
        value = dot(by_row, zc_in[k].reshape(count, size), 1, 0).astype(BF16)
        spread_rows(value, yb_out.at[0], rows_of[k], 0, tk)
        return x_send(yb_out.at[0], yb_in.at[0], a_rows, pieces[k])

    there.append(forward(0, 0, pieces[1], a_here[1]))
    mixed = []
    for k in range(PIECES):
        mixed.append(multiply(k, there[k]))
        if k + 2 < PIECES:
            there.append(forward(0, 0, pieces[k + 2], a_here[k + 2]))

    a_here, home = [], [turn(0, mixed[0])]
    for k, lanes in enumerate(pieces):
        if k + 1 < PIECES:
            home.append(turn(k + 1, mixed[k + 1]))
        arrive(home[k])
        v = update_stream(0, lanes, stream, yb_in.at[0], out_weights)
        stream[:, lanes] = v
        normed[:, lanes] = layer_norm(v.astype(F32)).astype(BF16)
        project(1, lanes, 0, normed, 0)
        a_here.append(send_w(1, a_in, lanes))
        by_columns(normed, normed_c, rows_of[k])
    b_here = []
    for lanes in pieces:
        project(1, lanes, 1, normed_c, 1)
        b_here.append(send_w(1, b_in, lanes))
    by_columns(stream, stream_c, rows_all)
    for lanes in pieces:
        set_gate(1, lanes, normed_c)
    there = [forward(1, 0, pieces[k], a_here[k]) for k in range(PIECES)]
    for k in range(PIECES):
        arrive(there[k])
        gather_rows(y_in.at[1], left.at[k * count : (k + 1) * count], rows_of[k], a_rows, 0, tk)
        turned[:, k * count : (k + 1) * count] = dot(order, left[k * count : (k + 1) * count], 1, 1).astype(BF16)
    there = [forward(1, 1, pieces[0], b_here[0])]

    def multiply(q, arrivals):
        arrive(arrivals)
        for k in range(PIECES):
            gather_rows(y_in.at[1], right_c.at[q, k * count : (k + 1) * count], rows_of[k], b_rows, q * step, part)
        value = dot(turned[...], right_c[q], 1, 0).astype(BF16)
        spread_rows(value, yb_out.at[1], rows_all, q * step, part)
        return x_send(yb_out.at[1], yb_in.at[1], a_rows, pieces[q])

    def forward_b(q):
        return forward(1, 1, pieces[q], b_here[q])

    home = in_steps(forward_b, multiply, go_back, there[0])

    for q, lanes in enumerate(pieces):
        arrive(home[q])
        base = update_stream(1, lanes, stream_c, wb_in, tri_out_ref[1]).astype(F32)
        v = layer_norm(base).astype(BF16)
        inner = dot(trans_in_ref[...], v, 0, 0)
        act = (jax.nn.silu(inner[:ffn]) * inner[ffn:]).astype(BF16)
        update = dot(trans_out_ref[...], act, 0, 0)
        result = (base + keep[1:2, lanes] * update).T.astype(BF16)
        cols = slice(q * part, (q + 1) * part)
        out_ref[:, cols, :] = result.reshape(ti, part, chan)
        store = pltpu.make_async_copy(out_ref.at[:, cols, :], out_hbm.at[:, cols, :], stores.at[q])
        store.start()
        started.append(store)

    for copies in started:
        copies.wait()


def body(pair, token_count, tri_in, tri_gate, tri_out, trans_in, trans_out):
    ti, tk, chan = pair.shape
    hidden = tri_out.shape[1]
    nz, nx = lax.axis_size("row_0"), lax.axis_size("col")
    np_ = CORES * nx
    tile, size = ti * tk, nx * tk
    hbm = pl.BlockSpec(memory_space=pltpu.HBM)
    given = (pair.reshape(tile, chan), tri_in, tri_gate, tri_out, trans_in, trans_out)
    sem = pltpu.SemaphoreType.DMA

    def buffers(*shape):
        return [pltpu.VMEM(shape, BF16)] * 2

    z_banks, x_banks = 6 * PIECES, 1 + 5 * PIECES
    return pl.pallas_call(
        functools.partial(kernel, (nz, nx, ti, tk)),
        out_shape=jax.ShapeDtypeStruct((ti, tk, chan), BF16),
        in_specs=[pl.BlockSpec(memory_space=pltpu.SMEM)] + [hbm] * len(given),
        out_specs=hbm,
        scratch_shapes=[
            pltpu.VMEM((ti, tk, chan), BF16), sem((PIECES,)),
            *[pltpu.VMEM(v.shape, v.dtype) for v in given], sem((len(given),)),
            *buffers(chan, tile),
            *buffers(chan, tile),
            pltpu.VMEM((chan, tile), F32),
            pltpu.VMEM((2, tile), F32),
            *buffers(size, size),
            pltpu.VMEM((size, size), BF16),
            pltpu.VMEM((PIECES, size, size // PIECES), BF16),
            *buffers(2, nz, 2 * np_, tile),
            *buffers(2, np_, 2 * nz, tile),
            *buffers(2, np_, nz, tile),
            *buffers(nz, np_, tile),
            *buffers(PIECES, nz, size // PIECES // nz, size),
            sem((z_banks,)), sem((z_banks,)), sem((x_banks,)), sem((x_banks,)),
        ],
        compiler_params=pltpu.CompilerParams(
            collective_id=0, has_side_effects=True, vmem_limit_bytes=56 * 1024 * 1024
        ),
        name="pairformer_block",
    )(token_count, *given)


def solution(mesh):
    torus = Mesh(
        mesh.devices.reshape(mesh.shape["grp"], mesh.shape["row"] // CORES, CORES, mesh.shape["col"]),
        ("grp", "row_0", "row_1", "col"),
    )
    grp_row = ("grp", "row_0", "row_1")
    placed = (P(grp_row, "col", None), P("grp"), P(), P(), P(), P(), P())
    return jax.shard_map(
        body, mesh=torus, in_specs=placed, out_specs=P(grp_row, "col", None), check_vma=False
    )
```
